256 devices in a mesh: src: 8 (over x, core), gauge: 32 (over y, z).
Axes of the slice: x: 4, y: 4, z: 8, core: 2. Of those that a mesh axis runs over, the one named last changes fastest.
Arguments:
- green: bfloat16 [512, 512, 4096], P('gauge', None, 'src'), may hold values from -0.1171875 to 0.1171875
- observed: float32 [128, 512, 512], P(None, 'gauge'), may hold values from -8 to 8
- gauge_mask: int32 [512], P('gauge'), may hold values 0 or 1
- source_mask: int32 [4096], P('src'), may hold values 0 or 1
Outputs:
- slip: float32 [128, 4096], P(None, 'src')
- residual: float32 [128, 512, 512], P(None, 'gauge')
The draws below stay inside these ranges and needn't reach their ends.
All inputs are finite; a program needn't handle non-finite values. No bound on the sum of `gauge_mask` or of `source_mask` on one device may be relied on, other than what follows from the above.
Results may differ from the reference program's by a relative error of at most 0.023.
Values may be sent and summed in bfloat16 or wider, within the bound.
No kernel may reach another device: no remote copies, remote signals or barrier semaphores. Data moves between devices by JAX's collectives and lax.ppermute only.
A program may use at most 64 MiB of HBM per device.

```python
import jax
import jax.numpy as jnp
from jax import lax

S = 4096
T_SIZE = 512
K = 128
ITERS = 3
GAUGES = 512
N_SRC = 8


def shared_green(key):
    place = jnp.arange(GAUGES, dtype=jnp.float32) / max(GAUGES - 1, 1)
    value_key = jax.random.fold_in(key, 11)
    column_key = jax.random.fold_in(key, 12)
    values = jnp.clip(jax.random.normal(value_key, (GAUGES, T_SIZE, S), jnp.float32), -6.0, 6.0)
    rising = 10.0 ** (0.5 * place)
    columns = jnp.exp(jax.random.uniform(column_key, (S,), jnp.float32, -2.302585, 0.0))
    scaled = values * (rising * (GAUGES * T_SIZE) ** (-0.5))[:, None, None] * columns[None, None, :]
    return (scaled.astype(jnp.bfloat16), columns)


def draw_green(key, part):
    green, columns = shared_green(key)
    return green


def draw_observed(key, part):
    green, columns = shared_green(key)
    slip_key = jax.random.fold_in(key, 13)
    noise_key = jax.random.fold_in(key, 14)
    amplitude = jax.random.normal(slip_key, (K, S), jnp.float32) / columns[None, :]
    signal = lax.dot_general(amplitude.astype(jnp.bfloat16), green, (((1,), (2,)), ((), ())), preferred_element_type=jnp.float32)
    signal = signal * lax.rsqrt(jnp.mean(signal * signal) + 1e-12)
    noise = jax.random.normal(noise_key, (K, GAUGES, T_SIZE), jnp.float32)
    return jnp.clip(signal + 0.05 * noise, -8.0, 8.0)


def set_ends(values, own_key, least, top_value):
    spot = [jax.random.randint(jax.random.fold_in(own_key, axis), (), 0, length) for axis, length in enumerate(values.shape)]
    widest = values.shape.index(max(values.shape))
    beside = spot[:widest] + [(spot[widest] + 1) % values.shape[widest]] + spot[widest + 1:]
    return values.at[tuple(spot)].set(least).at[tuple(beside)].set(top_value)


def setup_inputs(seed: int = 0) -> dict:
    streams_of = jax.random.split(jax.random.key(seed), 5)
    green = draw_green(jax.random.fold_in(streams_of[4], 71), 0)
    observed = draw_observed(jax.random.fold_in(streams_of[4], 71), 0)
    gauge_mask = set_ends((jax.random.randint(streams_of[2], (GAUGES,), 0, 8) < 7).astype(jnp.int32), jax.random.fold_in(streams_of[2], 1), 0, 1)
    source_mask = set_ends((jax.random.randint(streams_of[3], (S,), 0, 4) < 3).astype(jnp.int32), jax.random.fold_in(streams_of[3], 1), 0, 1)
    return {"green": green, "observed": observed, "gauge_mask": gauge_mask, "source_mask": source_mask}


def forward(green, vector, wg):
    width = green.shape[2] // N_SRC
    total = jnp.zeros((vector.shape[0], green.shape[0], green.shape[1]), jnp.float32)
    for block in range(N_SRC):
        piece = green[:, :, block * width:(block + 1) * width]
        rows = vector[:, block * width:(block + 1) * width]
        part = lax.dot_general(rows, piece, (((1,), (2,)), ((), ())), preferred_element_type=jnp.float32)
        rounded = lax.optimization_barrier(part.astype(jnp.bfloat16))
        total = total + rounded.astype(jnp.float32)
    return wg * total


def adjoint(green, wave, ps):
    out = lax.dot_general(wave, green, (((1, 2), (0, 1)), ((), ())), preferred_element_type=jnp.float32)
    return ps * out


def reference(green, observed, gauge_mask, source_mask):
    wg = gauge_mask.astype(jnp.float32)[None, :, None]
    ps = source_mask.astype(jnp.float32)[None, :]
    residual = wg * observed
    slip = jnp.zeros((observed.shape[0], green.shape[2]), jnp.float32)
    grad = adjoint(green, residual.astype(jnp.bfloat16), ps)
    direction = grad
    gamma = jnp.sum(grad * grad, axis=1)
    for step in range(ITERS):
        predicted = forward(green, direction.astype(jnp.bfloat16), wg)
        curvature = jnp.sum(predicted * predicted, axis=(1, 2))
        alpha = gamma / curvature
        slip = slip + alpha[:, None] * direction
        residual = residual - alpha[:, None, None] * predicted
        if step + 1 < ITERS:
            grad = adjoint(green, residual.astype(jnp.bfloat16), ps)
            fresh = jnp.sum(grad * grad, axis=1)
            direction = grad + (fresh / gamma)[:, None] * direction
            gamma = fresh
    return slip, residual
```

```python
import jax
import jax.numpy as jnp
from jax import lax
from jax.experimental import pallas as pl
from jax.experimental.pallas import tpu as pltpu
from jax.sharding import Mesh
from jax.sharding import PartitionSpec as P


BF = jnp.bfloat16
F32 = jnp.float32
NX, NC, NY, NZ = 4, 2, 4, 8
BLOCKS = NX * NC
LANES = 128
GAUGE = ("y", "z")


def moved(value, axis, count, step):
    pairs = [(i, (i + step) % count) for i in range(count)]
    return lax.ppermute(value, axis, pairs)


def total_of(parts):
    total = parts[0].astype(F32)
    for part in parts[1:]:
        total = total + part.astype(F32)
    return total


def call(body, grid, in_specs, out_specs, out_shape, scratch=(), scalars=0, limit=20):
    return pl.pallas_call(
        body,
        grid_spec=pltpu.PrefetchScalarGridSpec(
            num_scalar_prefetch=scalars,
            grid=grid,
            in_specs=in_specs,
            out_specs=out_specs,
            scratch_shapes=list(scratch),
        ),
        out_shape=out_shape,
        compiler_params=pltpu.CompilerParams(vmem_limit_bytes=limit * 2**20),
    )


def reordered(observed, mask, order):
    rows, gauges, times = observed.shape[0] // BLOCKS, observed.shape[1], observed.shape[2]

    def body(order_ref, obs_ref, mask_ref, wave_ref):
        value = obs_ref[...] * mask_ref[...][None, :, :1]
        wave_ref[0] = jnp.swapaxes(value, 0, 1).astype(BF)

    return call(
        body,
        (BLOCKS,),
        [
            pl.BlockSpec((rows, gauges, times), lambda i, o: (o[i], 0, 0)),
            pl.BlockSpec((gauges, LANES), lambda i, o: (0, 0)),
        ],
        pl.BlockSpec((1, gauges, rows, times), lambda i, o: (i, 0, 0, 0)),
        jax.ShapeDtypeStruct((BLOCKS, gauges, rows, times), BF),
        scalars=1,
    )(order, observed, mask)


def project(vector, green, start, gauges, step=4):
    _, times, width = green.shape
    rows = vector.shape[0] // BLOCKS
    first = start // step

    def body(vec_ref, green_ref, near_ref, far_ref):
        for g in range(step):
            part = lax.dot_general(
                vec_ref[...], green_ref[g], (((1,), (1,)), ((), ())), preferred_element_type=F32
            ).astype(BF)
            part = part.reshape(BLOCKS, rows, times)
            near_ref[:, g] = part[:NX]
            far_ref[:, g] = part[NX:]

    out = pl.BlockSpec((NX, step, rows, times), lambda i: (0, i, 0, 0))
    shape = jax.ShapeDtypeStruct((NX, gauges, rows, times), BF)
    return call(
        body,
        (gauges // step,),
        [
            pl.BlockSpec(vector.shape, lambda i: (0, 0)),
            pl.BlockSpec((step, times, width), lambda i: (first + i, 0, 0)),
        ],
        [out, out],
        [shape, shape],
    )(vector, green)


def split_two(value):
    high = value.astype(BF)
    return high, (value - high.astype(F32)).astype(BF)


def packed(sums):
    lane = lax.broadcasted_iota(jnp.int32, (sums[0].shape[0], LANES), 1)
    out = jnp.zeros(lane.shape, F32)
    for n, value in enumerate(sums):
        high, low = split_two(value)
        out = jnp.where(lane == 2 * n, high.astype(F32), out)
        out = jnp.where(lane == 2 * n + 1, low.astype(F32), out)
    return out


def gradient_parts(waves, green, start, gauges, others=(), carry=None, last=True, step=4):
    _, times, width = green.shape
    first = start // step
    stacked = lambda a: not isinstance(a, list)
    rows = waves.shape[2] if stacked(waves) else waves[0].shape[1]
    events = BLOCKS * rows
    count = 1 + len(others) if others else 0
    args, specs = [], []

    def add(a):
        at = len(args)
        if stacked(a):
            args.append(a)
            specs.append(pl.BlockSpec((BLOCKS, step, rows, times), lambda i: (0, first + i, 0, 0)))
            return lambda refs, s, g: refs[at][s, g]
        args.extend(a)
        specs.extend([pl.BlockSpec((step, rows, times), lambda i: (i, 0, 0)) for _ in a])
        return lambda refs, s, g: refs[at + s][g]

    read = add(waves)
    reads = [add(a) for a in others]
    green_at = len(args)
    args.append(green)
    specs.append(pl.BlockSpec((step, times, width), lambda i: (first + i, 0, 0)))
    carry_at = len(args)
    acc_shape, sum_shape = (events, width), (max(count, 1), events, LANES)
    if carry is not None:
        args.extend(carry)
        specs.append(pl.BlockSpec(acc_shape, lambda i: (0, 0)))
        specs.append(pl.BlockSpec(sum_shape, lambda i: (0, 0, 0)))
    total = len(args)

    def body(*refs):
        if last:
            out_ref, acc_ref, sum_ref = refs[total:]
        else:
            acc_ref, sum_ref = refs[total:]

        @pl.when(pl.program_id(0) == 0)
        def _():
            if carry is not None:
                acc_ref[...] = refs[carry_at][...]
                sum_ref[...] = refs[carry_at + 1][...]
            else:
                acc_ref[...] = jnp.zeros_like(acc_ref)
                sum_ref[...] = jnp.zeros_like(sum_ref)

        acc = acc_ref[...]
        for g in range(step):
            wave = jnp.concatenate([read(refs, s, g) for s in range(BLOCKS)], axis=0)
            acc = acc + lax.dot_general(
                wave, refs[green_at][g], (((1,), (0,)), ((), ())), preferred_element_type=F32
            )
        acc_ref[...] = acc
        if count:
            for s in range(BLOCKS):
                tot = [jnp.zeros((rows, LANES), F32) for _ in range(count)]
                for g in range(step):
                    u = read(refs, s, g).astype(F32)
                    for n in range(count):
                        v = u * (u if n == 0 else reads[n - 1](refs, s, g).astype(F32))
                        for t in range(times // LANES):
                            tot[n] = tot[n] + v[:, t * LANES : (t + 1) * LANES]
                for n in range(count):
                    sum_ref[n, s * rows : (s + 1) * rows, :] += tot[n]

        if last:

            @pl.when(pl.program_id(0) == gauges // step - 1)
            def _():
                out_ref[:, :width] = acc_ref[...].astype(BF)
                if count:
                    sums = [jnp.sum(sum_ref[n], axis=1, keepdims=True) for n in range(count)]
                    out_ref[:, width:] = packed(sums).astype(BF)

    acc_out = jax.ShapeDtypeStruct(acc_shape, F32)
    sum_out = jax.ShapeDtypeStruct(sum_shape, F32)
    wide = width + (LANES if count else 0)
    if last:
        out_specs = pl.BlockSpec((events, wide), lambda i: (0, 0))
        out_shape = jax.ShapeDtypeStruct((events, wide), BF)
        scratch = [pltpu.VMEM(acc_shape, F32), pltpu.VMEM(sum_shape, F32)]
    else:
        out_specs = [
            pl.BlockSpec(acc_shape, lambda i: (0, 0)),
            pl.BlockSpec(sum_shape, lambda i: (0, 0, 0)),
        ]
        out_shape = [acc_out, sum_out]
        scratch = []
    return call(body, (gauges // step,), specs, out_specs, out_shape, scratch=scratch)(*args)


def sent_to_all(value, axes, count):
    wide = jnp.broadcast_to(value[None], (count, *value.shape))
    return lax.all_to_all(wide, axes, 0, 0, tiled=True)


def gauge_sum(parts):
    count = NY * NZ
    pieces = parts.reshape(count, parts.shape[0] // count, parts.shape[1])
    got = lax.all_to_all(pieces, GAUGE, 0, 0, tiled=True)
    whole = sent_to_all(jnp.sum(got.astype(F32), axis=0), GAUGE, count)
    return whole.reshape(parts.shape)


def source_sum(near, far, mask):
    other = moved(far, "core", NC, 1)
    mine = [near[s].astype(F32) + other[s].astype(F32) for s in range(NX)]
    got = [mine[0]] + [moved(mine[s].astype(BF), "x", NX, -s) for s in range(1, NX)]
    return (mask * total_of(got)).astype(BF)


def spread(own):
    near = [own] + [moved(own, "x", NX, s) for s in range(1, NX)]
    return near + [moved(value, "core", NC, 1) for value in near]


NAMES = ("grad", "step", "direction", "slip", "facts")


def renewed(stage, summed, mask, state, width):
    events = summed.shape[0]
    lanes = ((0, width),) if stage == 0 else ((0, width), (width, width + LANES))

    def body(*refs):
        refs = list(refs)
        sum_ref, mask_ref = refs.pop(0), refs.pop(0)
        ins = dict(zip(NAMES, [refs.pop(0) for _ in NAMES])) if stage > 1 else {}
        if stage == 1:
            ins = {"grad": refs.pop(0)}
        out_bf = refs.pop(0)
        outs = dict(zip(NAMES, refs))
        got = sum_ref[:, :width] * mask_ref[...]
        if stage == 0:
            out_bf[...] = got.astype(BF)
            outs["grad"][...] = got
            return
        tail = sum_ref[:, width:]
        sums = [tail[:, 2 * n : 2 * n + 1] + tail[:, 2 * n + 1 : 2 * n + 2] for n in range(3)]
        grad = ins["grad"][...]
        if stage == 1:
            curvature, gamma = sums[0], sums[1]
            alpha = gamma / curvature
            beta = jnp.zeros_like(alpha)
            first, second = alpha, beta
            step, direction = got, grad
            slip = alpha * direction
        else:
            facts = ins["facts"][...]
            gamma = sums[1] - facts[:, 2:3] * sums[2]
            beta = gamma / facts[:, 0:1]
            curvature = sums[0] + 2.0 * beta * sums[2] + beta * beta * facts[:, 1:2]
            alpha = gamma / curvature
            first, second = facts[:, 2:3] + alpha * beta, alpha
            step = got + beta * ins["step"][...]
            direction = grad + beta * ins["direction"][...]
            slip = ins["slip"][...] + alpha * direction
        fresh = grad - alpha * step
        out_bf[...] = fresh.astype(BF)
        for name, value in zip(NAMES, (fresh, step, direction, slip)):
            outs[name][...] = value
        lane = lax.broadcasted_iota(jnp.int32, (events, LANES), 1)
        out = jnp.zeros((events, LANES), F32)
        for n, value in enumerate((gamma, curvature, first, second, beta)):
            out = jnp.where(lane == n, value, out)
        outs["facts"][...] = out

    wide = jax.ShapeDtypeStruct((events, width), F32)
    shapes = [jax.ShapeDtypeStruct((events, width), BF), wide]
    if stage:
        shapes += [wide] * 3 + [jax.ShapeDtypeStruct((events, LANES), F32)]
    args = [summed, mask]
    if stage == 1:
        args.append(state["grad"])
    elif stage:
        args += [state[n] for n in NAMES]
    whole = lambda a: pl.BlockSpec(a.shape, lambda i: (0,) * len(a.shape))
    outs = call(body, (1,), [whole(a) for a in args], [whole(s) for s in shapes], shapes)(*args)
    return outs[0], dict(zip(NAMES, outs[1:]))


def finished(places, news, observed, mask, waves, state):
    events, gauges, times = observed.shape
    rows = events // BLOCKS
    width = state["slip"].shape[1]
    halves = len(waves[0])
    each = gauges // halves

    def body(place_ref, new_ref, fact_ref, obs_ref, mask_ref, grad_ref, dir_ref, slip_ref, *refs):
        wave_refs, (out_slip, out_res) = refs[: 3 * halves], refs[3 * halves :]
        alpha, beta = new_ref[0, :, 0:1], new_ref[0, :, 1:2]
        old = fact_ref[...]
        second = old[:, 3:4] + alpha * beta
        first = old[:, 2:3] + alpha * beta * old[:, 4:5]
        out_slip[...] = slip_ref[...] + alpha * (grad_ref[...] + beta * dir_ref[...])
        for h in range(halves):
            value = 0.0
            for n, factor in enumerate((first, second, alpha)):
                value = value + factor[None] * wave_refs[n * halves + h][0].astype(F32)
            cut = slice(h * each, (h + 1) * each)
            out_res[:, cut] = obs_ref[:, cut] * mask_ref[cut][None, :, :1] - jnp.swapaxes(value, 0, 1)

    moving = lambda *shape: pl.BlockSpec(shape, lambda i, p: (p[i],) + (0,) * (len(shape) - 1))
    still = lambda *shape: pl.BlockSpec(shape, lambda i, p: (i,) + (0,) * (len(shape) - 1))
    small = moving(rows, width)
    flat = [half for wave in waves for half in wave]
    return call(
        body,
        (BLOCKS,),
        [
            still(1, rows, LANES),
            moving(rows, LANES),
            still(rows, gauges, times),
            pl.BlockSpec((gauges, LANES), lambda i, p: (0, 0)),
            small,
            small,
            small,
        ]
        + [moving(1, each, rows, times) for _ in flat],
        [still(rows, width), still(rows, gauges, times)],
        [
            jax.ShapeDtypeStruct((events, width), F32),
            jax.ShapeDtypeStruct((events, gauges, times), F32),
        ],
        scalars=1,
    )(places, news, state["facts"], observed, mask, state["grad"], state["direction"], state["slip"], *flat)


HALVES = 2


def per_device(green, observed, gauge_mask, source_mask):
    x, core = lax.axis_index("x"), lax.axis_index("core")
    gauges, times, width = green.shape
    each = gauges // HALVES
    place = jnp.arange(BLOCKS, dtype=jnp.int32)
    order = (x - place % NX) % NX * NC + (core + place // NX) % NC
    places = (core + place % NC) % NC * NX + (x - place // NC) % NX

    wg = gauge_mask.astype(F32)
    wide_mask = jnp.broadcast_to(wg[:, None], (gauges, LANES))
    ps = source_mask.astype(F32)[None, :]

    def predicted(vector):
        owns, waves = [], []
        parts = [project(vector, green, h * each, each) for h in range(HALVES)]
        for h in range(HALVES):
            own = source_sum(*parts[h], wg[h * each : (h + 1) * each, None, None])
            owns.append(own)
            waves.append(spread(own))
        return owns, waves

    def gradient(waves, others):
        carry = None
        for h in range(HALVES):
            carry = gradient_parts(
                waves[h],
                green,
                h * each,
                each,
                [a if not isinstance(a, list) else a[h] for a in others],
                carry,
                h == HALVES - 1,
            )
        return gauge_sum(carry)

    start = reordered(observed, wide_mask, order)
    summed = gauge_sum(gradient_parts(start, green, 0, gauges))
    vector, state = renewed(0, summed, ps, None, width)

    _, first = predicted(vector)
    vector, state = renewed(1, gradient(first, [start]), ps, state, width)
    _, second = predicted(vector)
    vector, state = renewed(2, gradient(second, [start, first]), ps, state, width)
    owns, third = predicted(vector)

    sums = 0.0
    for h in range(HALVES):
        wave = owns[h].astype(F32)
        cut = slice(h * each, (h + 1) * each)
        others = (owns[h], start[0, cut], first[h][0], second[h][0])
        sums = sums + jnp.stack([jnp.sum(wave * o.astype(F32), axis=(0, 2)) for o in others])
    sums = jnp.sum(sent_to_all(sums, GAUGE, NY * NZ), axis=0)
    rows = sums.shape[1]
    past = [state["facts"][:rows, n] for n in range(5)]
    gamma = sums[1] - past[2] * sums[2] - past[3] * sums[3]
    beta = gamma / past[0]
    along = sums[3] + past[4] * sums[2]
    alpha = gamma / (sums[0] + 2.0 * beta * along + beta * beta * past[1])
    news = sent_to_all(jnp.stack([alpha, beta]), ("x", "core"), BLOCKS)
    news = jnp.pad(news.transpose(0, 2, 1), ((0, 0), (0, 0), (0, LANES - 2)))
    stacks = [[jnp.stack(half) for half in wave] for wave in (first, second, third)]
    return tuple(finished(places, news, observed, wide_mask, stacks, state))


def solution(mesh):
    finer = Mesh(mesh.devices.reshape(NX, NC, NY, NZ), ("x", "core", "y", "z"))
    src = ("x", "core")
    in_specs = (P(GAUGE, None, src), P(None, GAUGE, None), P(GAUGE), P(src))
    out_specs = (P(None, src), P(None, GAUGE, None))
    return jax.shard_map(
        per_device, mesh=finer, in_specs=in_specs, out_specs=out_specs, check_vma=False
    )
```

```python
import jax
import jax.numpy as jnp
from jax import lax
from jax.experimental import pallas as pl
from jax.experimental.pallas import tpu as pltpu
from jax.sharding import Mesh
from jax.sharding import PartitionSpec as P


BF = jnp.bfloat16
F32 = jnp.float32
NX, NC, NY, NZ = 4, 2, 4, 8
BLOCKS = NX * NC
LANES = 128
GAUGE = ("y", "z")
PIECES = NY * NZ


def moved(value, axis, count, step):
    pairs = [(i, (i + step) % count) for i in range(count)]
    return lax.ppermute(value, axis, pairs)


def total_of(parts):
    total = parts[0].astype(F32)
    for part in parts[1:]:
        total = total + part.astype(F32)
    return total


def call(body, grid, in_specs, out_specs, out_shape, scratch=(), scalars=0, limit=20):
    return pl.pallas_call(
        body,
        grid_spec=pltpu.PrefetchScalarGridSpec(
            num_scalar_prefetch=scalars,
            grid=grid,
            in_specs=in_specs,
            out_specs=out_specs,
            scratch_shapes=list(scratch),
        ),
        out_shape=out_shape,
        compiler_params=pltpu.CompilerParams(vmem_limit_bytes=limit * 2**20),
    )


def reordered(observed, mask, order):
    rows, gauges, times = observed.shape[0] // BLOCKS, observed.shape[1], observed.shape[2]

    def body(order_ref, obs_ref, mask_ref, wave_ref):
        value = obs_ref[...] * mask_ref[...][None, :, :1]
        wave_ref[0] = jnp.swapaxes(value, 0, 1).astype(BF)

    return call(
        body,
        (BLOCKS,),
        [
            pl.BlockSpec((rows, gauges, times), lambda i, o: (o[i], 0, 0)),
            pl.BlockSpec((gauges, LANES), lambda i, o: (0, 0)),
        ],
        pl.BlockSpec((1, gauges, rows, times), lambda i, o: (i, 0, 0, 0)),
        jax.ShapeDtypeStruct((BLOCKS, gauges, rows, times), BF),
        scalars=1,
    )(order, observed, mask)


def project(vector, green, start, gauges, step=4):
    _, times, width = green.shape
    rows = vector.shape[0] // BLOCKS
    first = start // step

    def body(vec_ref, green_ref, near_ref, far_ref):
        for g in range(step):
            part = lax.dot_general(
                vec_ref[...], green_ref[g], (((1,), (1,)), ((), ())), preferred_element_type=F32
            ).astype(BF)
            part = part.reshape(BLOCKS, rows, times)
            near_ref[:, g] = part[:NX]
            far_ref[:, g] = part[NX:]

    out = pl.BlockSpec((NX, step, rows, times), lambda i: (0, i, 0, 0))
    shape = jax.ShapeDtypeStruct((NX, gauges, rows, times), BF)
    return call(
        body,
        (gauges // step,),
        [
            pl.BlockSpec(vector.shape, lambda i: (0, 0)),
            pl.BlockSpec((step, times, width), lambda i: (first + i, 0, 0)),
        ],
        [out, out],
        [shape, shape],
    )(vector, green)


def split_two(value):
    high = value.astype(BF)
    return high, (value - high.astype(F32)).astype(BF)


def packed(sums):
    lane = lax.broadcasted_iota(jnp.int32, (sums[0].shape[0], LANES), 1)
    out = jnp.zeros(lane.shape, F32)
    for n, value in enumerate(sums):
        high, low = split_two(value)
        out = jnp.where(lane == 2 * n, high.astype(F32), out)
        out = jnp.where(lane == 2 * n + 1, low.astype(F32), out)
    return out


def folded(value):
    cuts = [value[..., t : t + LANES] for t in range(0, value.shape[-1], LANES)]
    return total_of(cuts)


def gradient_parts(waves, green, start, gauges, others=(), carry=None, last=True, step=4):
    _, times, width = green.shape
    first = start // step
    stacked = lambda a: not isinstance(a, list)
    rows = waves.shape[2] if stacked(waves) else waves[0].shape[1]
    events = BLOCKS * rows
    count = 1 + len(others) if others else 0
    args, specs = [], []

    def add(a):
        at = len(args)
        if stacked(a):
            args.append(a)
            specs.append(pl.BlockSpec((BLOCKS, step, rows, times), lambda i: (0, first + i, 0, 0)))
            return lambda refs, s, g: refs[at][s, g]
        args.extend(a)
        specs.extend([pl.BlockSpec((step, rows, times), lambda i: (i, 0, 0)) for _ in a])
        return lambda refs, s, g: refs[at + s][g]

    read = add(waves)
    reads = [add(a) for a in others]
    green_at = len(args)
    args.append(green)
    specs.append(pl.BlockSpec((step, times, width), lambda i: (first + i, 0, 0)))
    carry_at = len(args)
    acc_shape, sum_shape = (events, width), (max(count, 1), events, LANES)
    if carry is not None:
        args.extend(carry)
        specs.append(pl.BlockSpec(acc_shape, lambda i: (0, 0)))
        specs.append(pl.BlockSpec(sum_shape, lambda i: (0, 0, 0)))
    total = len(args)

    def body(*refs):
        if last:
            out_ref, acc_ref, sum_ref = refs[total:]
        else:
            acc_ref, sum_ref = refs[total:]

        @pl.when(pl.program_id(0) == 0)
        def _():
            if carry is not None:
                acc_ref[...] = refs[carry_at][...]
                sum_ref[...] = refs[carry_at + 1][...]
            else:
                acc_ref[...] = jnp.zeros_like(acc_ref)
                sum_ref[...] = jnp.zeros_like(sum_ref)

        acc = acc_ref[...]
        for g in range(step):
            wave = jnp.concatenate([read(refs, s, g) for s in range(BLOCKS)], axis=0)
            acc = acc + lax.dot_general(
                wave, refs[green_at][g], (((1,), (0,)), ((), ())), preferred_element_type=F32
            )
        acc_ref[...] = acc
        if count:

            @pl.loop(0, step)
            def _(g):
                for s in range(BLOCKS):
                    u = read(refs, s, g).astype(F32)
                    for n in range(count):
                        v = u * (u if n == 0 else reads[n - 1](refs, s, g).astype(F32))
                        sum_ref[n, s * rows : (s + 1) * rows, :] += folded(v)

        if last:

            @pl.when(pl.program_id(0) == gauges // step - 1)
            def _():
                if count:
                    sums = [jnp.sum(sum_ref[n], axis=1, keepdims=True) for n in range(count)]
                    sum_ref[0] = packed(sums)
                for q in range(PIECES):
                    at = slice(q * events // PIECES, (q + 1) * events // PIECES)
                    out_ref[q, :, :width] = acc_ref[at, :].astype(BF)
                    if count:
                        out_ref[q, :, width:] = sum_ref[0, at, :].astype(BF)

    acc_out = jax.ShapeDtypeStruct(acc_shape, F32)
    sum_out = jax.ShapeDtypeStruct(sum_shape, F32)
    wide = width + (LANES if count else 0)
    if last:
        out_specs = pl.BlockSpec((PIECES, events // PIECES, wide), lambda i: (0, 0, 0))
        out_shape = jax.ShapeDtypeStruct((PIECES, events // PIECES, wide), BF)
        scratch = [pltpu.VMEM(acc_shape, F32), pltpu.VMEM(sum_shape, F32)]
    else:
        out_specs = [
            pl.BlockSpec(acc_shape, lambda i: (0, 0)),
            pl.BlockSpec(sum_shape, lambda i: (0, 0, 0)),
        ]
        out_shape = [acc_out, sum_out]
        scratch = []
    return call(body, (gauges // step,), specs, out_specs, out_shape, scratch=scratch)(*args)


def sent_to_all(value, axes, count):
    wide = jnp.broadcast_to(value[None], (count, *value.shape))
    return lax.all_to_all(wide, axes, 0, 0, tiled=True)


def gauge_sum(pieces):
    got = lax.all_to_all(pieces, GAUGE, 0, 0, tiled=True)
    return sent_to_all(jnp.sum(got.astype(F32), axis=0), GAUGE, PIECES)


def source_sum(near, far, mask):
    other = moved(far, "core", NC, 1)
    mine = [near[s].astype(F32) + other[s].astype(F32) for s in range(NX)]
    got = [mine[0]] + [moved(mine[s].astype(BF), "x", NX, -s) for s in range(1, NX)]
    return (mask * total_of(got)).astype(BF)


def spread(own):
    near = [own] + [moved(own, "x", NX, s) for s in range(1, NX)]
    return near + [moved(value, "core", NC, 1) for value in near]


NAMES = ("grad", "step", "direction", "slip", "facts")


def renewed(stage, summed, mask, state, width):
    pieces, share, total = summed.shape
    events = pieces * share

    def body(*refs):
        refs = list(refs)
        sum_ref, mask_ref = refs.pop(0), refs.pop(0)
        ins = dict(zip(NAMES, [refs.pop(0) for _ in NAMES])) if stage > 1 else {}
        if stage == 1:
            ins = {"grad": refs.pop(0)}
        out_bf = refs.pop(0)
        joined = refs.pop()
        outs = dict(zip(NAMES, refs))
        for q in range(pieces):
            joined[q * share : (q + 1) * share, :] = sum_ref[q]
        got = joined[:, :width] * mask_ref[...]
        if stage == 0:
            out_bf[...] = got.astype(BF)
            outs["grad"][...] = got
            return
        tail = joined[:, width:]
        sums = [tail[:, 2 * n : 2 * n + 1] + tail[:, 2 * n + 1 : 2 * n + 2] for n in range(3)]
        grad = ins["grad"][...]
        if stage == 1:
            curvature, gamma = sums[0], sums[1]
            alpha = gamma / curvature
            beta = jnp.zeros_like(alpha)
            first, second = alpha, beta
            step, direction = got, grad
            slip = alpha * direction
        else:
            facts = ins["facts"][...]
            gamma = sums[1] - facts[:, 2:3] * sums[2]
            beta = gamma / facts[:, 0:1]
            curvature = sums[0] + 2.0 * beta * sums[2] + beta * beta * facts[:, 1:2]
            alpha = gamma / curvature
            first, second = facts[:, 2:3] + alpha * beta, alpha
            step = got + beta * ins["step"][...]
            direction = grad + beta * ins["direction"][...]
            slip = ins["slip"][...] + alpha * direction
        fresh = grad - alpha * step
        out_bf[...] = fresh.astype(BF)
        for name, value in zip(NAMES, (fresh, step, direction, slip)):
            outs[name][...] = value
        lane = lax.broadcasted_iota(jnp.int32, (events, LANES), 1)
        out = jnp.zeros((events, LANES), F32)
        for n, value in enumerate((gamma, curvature, first, second, beta)):
            out = jnp.where(lane == n, value, out)
        outs["facts"][...] = out

    wide = jax.ShapeDtypeStruct((events, width), F32)
    shapes = [jax.ShapeDtypeStruct((events, width), BF), wide]
    if stage:
        shapes += [wide] * 3 + [jax.ShapeDtypeStruct((events, LANES), F32)]
    args = [summed, mask]
    if stage == 1:
        args.append(state["grad"])
    elif stage:
        args += [state[n] for n in NAMES]
    whole = lambda a: pl.BlockSpec(a.shape, lambda i: (0,) * len(a.shape))
    scratch = [pltpu.VMEM((events, total), F32)]
    outs = call(body, (1,), [whole(a) for a in args], [whole(s) for s in shapes], shapes, scratch=scratch)(*args)
    return outs[0], dict(zip(NAMES, outs[1:]))


def picked(place, waves, into):
    for at in range(BLOCKS):

        @pl.when(place == at)
        def _():
            for n, refs in enumerate(waves):
                into[n] = refs[at][...]


def whole_refs(flat):
    return [pl.BlockSpec(memory_space=pltpu.VMEM) for _ in flat]


def halfway(order, observed, mask, first, second, facts):
    events, gauges, times = observed.shape
    rows = events // BLOCKS
    halves = len(first)
    each = gauges // halves
    flat = [a for half in first + second for a in half]

    def body(order_ref, obs_ref, mask_ref, fact_ref, *refs):
        res_ref, wave_ref, block = refs[len(flat) :]
        groups = [refs[n * BLOCKS : (n + 1) * BLOCKS] for n in range(2 * halves)]
        picked(pl.program_id(0), groups, block)
        old = fact_ref[...]
        a, b, beta = old[:, 2:3], old[:, 3:4], old[:, 4:5]
        for h in range(halves):
            one, two = block[h].astype(F32), block[halves + h].astype(F32)
            cut = slice(h * each, (h + 1) * each)
            left = jnp.swapaxes(a[None] * one + b[None] * two, 0, 1)
            res_ref[:, cut] = obs_ref[:, cut] * mask_ref[cut][None, :, :1] - left
            wave_ref[:, cut] = jnp.swapaxes(two + beta[None] * one, 0, 1)

    natural = pl.BlockSpec((rows, gauges, times), lambda i, o: (o[i], 0, 0))
    shape = jax.ShapeDtypeStruct(observed.shape, F32)
    return call(
        body,
        (BLOCKS,),
        [
            natural,
            pl.BlockSpec((gauges, LANES), lambda i, o: (0, 0)),
            pl.BlockSpec((rows, LANES), lambda i, o: (i, 0)),
        ]
        + whole_refs(flat),
        [natural, natural],
        [shape, shape],
        scratch=[pltpu.VMEM((2 * halves, each, rows, times), BF)],
        scalars=1,
    )(order, observed, mask, facts, *flat)


def turned(value):
    spare = LANES - value.shape[0]
    if spare:
        value = jnp.concatenate([value, jnp.zeros((spare, LANES), F32)], axis=0)
    return value.T


def last_sums(owns, others, facts):
    rows = owns[0].shape[1]
    groups = [owns] + others

    def body(*refs):
        out_ref, sum_ref = refs[-2:]
        halves = len(owns)
        sum_ref[...] = jnp.zeros_like(sum_ref)
        for h in range(halves):
            u = refs[h][...].astype(F32)
            for n in range(len(groups)):
                v = u * (u if n == 0 else refs[n * halves + h][...].astype(F32))
                v = folded(jnp.sum(v, axis=0))
                lane = lax.broadcasted_iota(jnp.int32, (rows, LANES), 1)
                sum_ref[...] += jnp.where(lane == n, jnp.sum(v, axis=1, keepdims=True), 0.0)
        out_ref[...] = turned(sum_ref[...])[:8]

    flat = [a for group in groups for a in group]
    return call(
        body,
        (1,),
        [pl.BlockSpec(a.shape, lambda i: (0, 0, 0)) for a in flat],
        pl.BlockSpec((8, LANES), lambda i: (0, 0)),
        jax.ShapeDtypeStruct((8, LANES), F32),
        scratch=[pltpu.VMEM((rows, LANES), F32)],
    )(*flat)


def last_factors(sums, facts):
    def body(sum_ref, fact_ref, out_ref):
        tot = jnp.sum(sum_ref[...], axis=0)
        old = turned(fact_ref[...])
        row = lambda a, n: a[n : n + 1]
        gamma = row(tot, 1) - row(old, 2) * row(tot, 2) - row(old, 3) * row(tot, 3)
        beta = gamma / row(old, 0)
        along = row(tot, 3) + row(old, 4) * row(tot, 2)
        alpha = gamma / (row(tot, 0) + 2.0 * beta * along + beta * beta * row(old, 1))
        out_ref[...] = jnp.zeros_like(out_ref)
        out_ref[0:1] = alpha
        out_ref[1:2] = beta

    return call(
        body,
        (1,),
        [pl.BlockSpec(sums.shape, lambda i: (0, 0, 0)), pl.BlockSpec((16, LANES), lambda i: (0, 0))],
        pl.BlockSpec((8, LANES), lambda i: (0, 0)),
        jax.ShapeDtypeStruct((8, LANES), F32),
    )(sums, facts)


def finished(order, news, res, prior, waves, state):
    events, gauges, times = res.shape
    rows = events // BLOCKS
    width = state["slip"].shape[1]
    halves = len(waves)
    each = gauges // halves
    flat = [a for half in waves for a in half]

    def body(order_ref, new_ref, res_ref, prior_ref, grad_ref, dir_ref, slip_ref, *refs):
        out_slip, out_res, block = refs[len(flat) :]
        groups = [refs[n * BLOCKS : (n + 1) * BLOCKS] for n in range(halves)]
        picked(pl.program_id(0), groups, block)
        new = turned(new_ref[0])[:rows]
        alpha, beta = new[:, 0:1], new[:, 1:2]
        out_slip[...] = slip_ref[...] + alpha * (grad_ref[...] + beta * dir_ref[...])
        alpha, both = alpha[:, :, None], (alpha * beta)[:, :, None]
        for h in range(halves):
            cut = slice(h * each, (h + 1) * each)
            wave = jnp.swapaxes(block[h].astype(F32) * new[:, 0:1][None], 0, 1)
            out_res[:, cut] = res_ref[:, cut] - wave - both * prior_ref[:, cut]

    natural = pl.BlockSpec((rows, gauges, times), lambda i, o: (o[i], 0, 0))
    small = pl.BlockSpec((rows, width), lambda i, o: (i, 0))
    return call(
        body,
        (BLOCKS,),
        [pl.BlockSpec((1, 8, LANES), lambda i, o: (o[i], 0, 0)), natural, natural, small, small, small]
        + whole_refs(flat),
        [pl.BlockSpec((rows, width), lambda i, o: (o[i], 0)), natural],
        [
            jax.ShapeDtypeStruct((events, width), F32),
            jax.ShapeDtypeStruct((events, gauges, times), F32),
        ],
        scratch=[pltpu.VMEM((halves, each, rows, times), BF)],
        scalars=1,
    )(order, news, res, prior, state["grad"], state["direction"], state["slip"], *flat)


HALVES = 2


def per_device(green, observed, gauge_mask, source_mask):
    x, core = lax.axis_index("x"), lax.axis_index("core")
    gauges, times, width = green.shape
    each = gauges // HALVES
    place = jnp.arange(BLOCKS, dtype=jnp.int32)
    order = (x - place % NX) % NX * NC + (core + place // NX) % NC

    wg = gauge_mask.astype(F32)
    wide_mask = jnp.broadcast_to(wg[:, None], (gauges, LANES))
    ps = source_mask.astype(F32)[None, :]
    wg, wide_mask, ps, order = lax.optimization_barrier((wg, wide_mask, ps, order))

    def predicted(vector):
        owns, waves = [], []
        parts = [project(vector, green, h * each, each) for h in range(HALVES)]
        for h in range(HALVES):
            own = source_sum(*parts[h], wg[h * each : (h + 1) * each, None, None])
            owns.append(own)
            waves.append(spread(own))
        return owns, waves

    def gradient(waves, others):
        carry = None
        for h in range(HALVES):
            carry = gradient_parts(
                waves[h],
                green,
                h * each,
                each,
                [a if not isinstance(a, list) else a[h] for a in others],
                carry,
                h == HALVES - 1,
            )
        return gauge_sum(carry)

    start = reordered(observed, wide_mask, order)
    summed = gauge_sum(gradient_parts(start, green, 0, gauges))
    vector, state = renewed(0, summed, ps, None, width)

    _, first = predicted(vector)
    vector, state = renewed(1, gradient(first, [start]), ps, state, width)
    _, second = predicted(vector)
    vector, state = renewed(2, gradient(second, [start, first]), ps, state, width)
    owns, third = predicted(vector)

    res, prior = halfway(order, observed, wide_mask, first, second, state["facts"])
    others = [
        [start[0, h * each : (h + 1) * each] for h in range(HALVES)],
        [first[h][0] for h in range(HALVES)],
        [second[h][0] for h in range(HALVES)],
    ]
    sums = last_sums(owns, others, state["facts"])
    sums = sent_to_all(sums, GAUGE, PIECES)
    news = sent_to_all(last_factors(sums, state["facts"]), ("x", "core"), BLOCKS)
    return tuple(finished(order, news, res, prior, third, state))


def solution(mesh):
    finer = Mesh(mesh.devices.reshape(NX, NC, NY, NZ), ("x", "core", "y", "z"))
    src = ("x", "core")
    in_specs = (P(GAUGE, None, src), P(None, GAUGE, None), P(GAUGE), P(src))
    out_specs = (P(None, src), P(None, GAUGE, None))
    return jax.shard_map(
        per_device, mesh=finer, in_specs=in_specs, out_specs=out_specs, check_vma=False
    )
```

```python
import jax
import jax.numpy as jnp
from jax import lax
from jax.experimental import pallas as pl
from jax.experimental.pallas import tpu as pltpu
from jax.sharding import Mesh
from jax.sharding import PartitionSpec as P


BF = jnp.bfloat16
F32 = jnp.float32
NX, NC, NY, NZ = 4, 2, 4, 8
BLOCKS = NX * NC
LANES = 128
GAUGE = ("y", "z")
PIECES = NY * NZ


def moved(value, axis, count, step):
    pairs = [(i, (i + step) % count) for i in range(count)]
    return lax.ppermute(value, axis, pairs)


def total_of(parts):
    total = parts[0].astype(F32)
    for part in parts[1:]:
        total = total + part.astype(F32)
    return total


def call(body, grid, in_specs, out_specs, out_shape, scratch=(), scalars=0, limit=20):
    return pl.pallas_call(
        body,
        grid_spec=pltpu.PrefetchScalarGridSpec(
            num_scalar_prefetch=scalars,
            grid=grid,
            in_specs=in_specs,
            out_specs=out_specs,
            scratch_shapes=list(scratch),
        ),
        out_shape=out_shape,
        compiler_params=pltpu.CompilerParams(vmem_limit_bytes=limit * 2**20),
    )


def reordered(observed, mask, order):
    rows, gauges, times = observed.shape[0] // BLOCKS, observed.shape[1], observed.shape[2]

    def body(order_ref, obs_ref, mask_ref, wave_ref):
        value = obs_ref[...] * mask_ref[...][None, :, :1]
        wave_ref[0] = jnp.swapaxes(value, 0, 1).astype(BF)

    return call(
        body,
        (BLOCKS,),
        [
            pl.BlockSpec((rows, gauges, times), lambda i, o: (o[i], 0, 0)),
            pl.BlockSpec((gauges, LANES), lambda i, o: (0, 0)),
        ],
        pl.BlockSpec((1, gauges, rows, times), lambda i, o: (i, 0, 0, 0)),
        jax.ShapeDtypeStruct((BLOCKS, gauges, rows, times), BF),
        scalars=1,
    )(order, observed, mask)


def project(vector, green, start, gauges, step=4):
    _, times, width = green.shape
    rows = vector.shape[0] // BLOCKS
    first = start // step

    def body(vec_ref, green_ref, near_ref, far_ref):
        for g in range(step):
            part = lax.dot_general(
                vec_ref[...], green_ref[g], (((1,), (1,)), ((), ())), preferred_element_type=F32
            ).astype(BF)
            part = part.reshape(BLOCKS, rows, times)
            near_ref[:, g] = part[:NX]
            far_ref[:, g] = part[NX:]

    out = pl.BlockSpec((NX, step, rows, times), lambda i: (0, i, 0, 0))
    shape = jax.ShapeDtypeStruct((NX, gauges, rows, times), BF)
    return call(
        body,
        (gauges // step,),
        [
            pl.BlockSpec(vector.shape, lambda i: (0, 0)),
            pl.BlockSpec((step, times, width), lambda i: (first + i, 0, 0)),
        ],
        [out, out],
        [shape, shape],
    )(vector, green)


def split_two(value):
    high = value.astype(BF)
    return high, (value - high.astype(F32)).astype(BF)


def packed(sums):
    lane = lax.broadcasted_iota(jnp.int32, (sums[0].shape[0], LANES), 1)
    out = jnp.zeros(lane.shape, F32)
    for n, value in enumerate(sums):
        high, low = split_two(value)
        out = jnp.where(lane == 2 * n, high.astype(F32), out)
        out = jnp.where(lane == 2 * n + 1, low.astype(F32), out)
    return out


def folded(value):
    cuts = [value[..., t : t + LANES] for t in range(0, value.shape[-1], LANES)]
    return total_of(cuts)


def gradient_parts(waves, green, start, gauges, others=(), carry=None, last=True, step=4):
    _, times, width = green.shape
    first = start // step
    stacked = lambda a: not isinstance(a, list)
    rows = waves.shape[2] if stacked(waves) else waves[0].shape[1]
    events = BLOCKS * rows
    count = 1 + len(others) if others else 0
    args, specs = [], []

    def add(a):
        at = len(args)
        if stacked(a):
            args.append(a)
            specs.append(pl.BlockSpec((BLOCKS, step, rows, times), lambda i: (0, first + i, 0, 0)))
            return lambda refs, s, g: refs[at][s, g]
        args.extend(a)
        specs.extend([pl.BlockSpec((step, rows, times), lambda i: (i, 0, 0)) for _ in a])
        return lambda refs, s, g: refs[at + s][g]

    read = add(waves)
    reads = [add(a) for a in others]
    green_at = len(args)
    args.append(green)
    specs.append(pl.BlockSpec((step, times, width), lambda i: (first + i, 0, 0)))
    carry_at = len(args)
    acc_shape, sum_shape = (events, width), (max(count, 1), events, LANES)
    if carry is not None:
        args.extend(carry)
        specs.append(pl.BlockSpec(acc_shape, lambda i: (0, 0)))
        specs.append(pl.BlockSpec(sum_shape, lambda i: (0, 0, 0)))
    total = len(args)

    def body(*refs):
        if last:
            out_ref, acc_ref, sum_ref = refs[total:]
        else:
            acc_ref, sum_ref = refs[total:]

        @pl.when(pl.program_id(0) == 0)
        def _():
            if carry is not None:
                acc_ref[...] = refs[carry_at][...]
                sum_ref[...] = refs[carry_at + 1][...]
            else:
                acc_ref[...] = jnp.zeros_like(acc_ref)
                sum_ref[...] = jnp.zeros_like(sum_ref)

        acc = acc_ref[...]
        for g in range(step):
            wave = jnp.concatenate([read(refs, s, g) for s in range(BLOCKS)], axis=0)
            acc = acc + lax.dot_general(
                wave, refs[green_at][g], (((1,), (0,)), ((), ())), preferred_element_type=F32
            )
        acc_ref[...] = acc
        if count:

            @pl.loop(0, step)
            def _(g):
                for s in range(BLOCKS):
                    u = read(refs, s, g).astype(F32)
                    for n in range(count):
                        v = u * (u if n == 0 else reads[n - 1](refs, s, g).astype(F32))
                        sum_ref[n, s * rows : (s + 1) * rows, :] += folded(v)

        if last:

            @pl.when(pl.program_id(0) == gauges // step - 1)
            def _():
                if count:
                    sums = [jnp.sum(sum_ref[n], axis=1, keepdims=True) for n in range(count)]
                    sum_ref[0] = packed(sums)
                for q in range(PIECES):
                    at = slice(q * events // PIECES, (q + 1) * events // PIECES)
                    out_ref[q, :, :width] = acc_ref[at, :].astype(BF)
                    if count:
                        out_ref[q, :, width:] = sum_ref[0, at, :].astype(BF)

    acc_out = jax.ShapeDtypeStruct(acc_shape, F32)
    sum_out = jax.ShapeDtypeStruct(sum_shape, F32)
    wide = width + (LANES if count else 0)
    if last:
        out_specs = pl.BlockSpec((PIECES, events // PIECES, wide), lambda i: (0, 0, 0))
        out_shape = jax.ShapeDtypeStruct((PIECES, events // PIECES, wide), BF)
        scratch = [pltpu.VMEM(acc_shape, F32), pltpu.VMEM(sum_shape, F32)]
    else:
        out_specs = [
            pl.BlockSpec(acc_shape, lambda i: (0, 0)),
            pl.BlockSpec(sum_shape, lambda i: (0, 0, 0)),
        ]
        out_shape = [acc_out, sum_out]
        scratch = []
    return call(body, (gauges // step,), specs, out_specs, out_shape, scratch=scratch)(*args)


def sent_to_all(value, axes, count):
    wide = jnp.broadcast_to(value[None], (count, *value.shape))
    return lax.all_to_all(wide, axes, 0, 0, tiled=True)


def gauge_sum(pieces):
    got = lax.all_to_all(pieces, GAUGE, 0, 0, tiled=True)
    return sent_to_all(jnp.sum(got.astype(F32), axis=0), GAUGE, PIECES)


def source_sum(near, far, mask):
    other = moved(far, "core", NC, 1)
    mine = [near[s].astype(F32) + other[s].astype(F32) for s in range(NX)]
    got = [mine[0]] + [moved(mine[s].astype(BF), "x", NX, -s) for s in range(1, NX)]
    return (mask * total_of(got)).astype(BF)


def along_x(own):
    return [own] + [moved(own, "x", NX, s) for s in range(1, NX)]


def with_core(near):
    return near + [moved(value, "core", NC, 1) for value in near]


NAMES = ("grad", "step", "direction", "slip", "facts")


def renewed(stage, summed, mask, state, width):
    pieces, share, total = summed.shape
    events = pieces * share

    def body(*refs):
        refs = list(refs)
        sum_ref, mask_ref = refs.pop(0), refs.pop(0)
        ins = dict(zip(NAMES, [refs.pop(0) for _ in NAMES])) if stage > 1 else {}
        if stage == 1:
            ins = {"grad": refs.pop(0)}
        out_bf = refs.pop(0)
        joined = refs.pop()
        outs = dict(zip(NAMES, refs))
        for q in range(pieces):
            joined[q * share : (q + 1) * share, :] = sum_ref[q]
        got = joined[:, :width] * mask_ref[...]
        if stage == 0:
            out_bf[...] = got.astype(BF)
            outs["grad"][...] = got
            return
        tail = joined[:, width:]
        sums = [tail[:, 2 * n : 2 * n + 1] + tail[:, 2 * n + 1 : 2 * n + 2] for n in range(3)]
        grad = ins["grad"][...]
        if stage == 1:
            curvature, gamma = sums[0], sums[1]
            alpha = gamma / curvature
            beta = jnp.zeros_like(alpha)
            first, second = alpha, beta
            step, direction = got, grad
            slip = alpha * direction
        else:
            facts = ins["facts"][...]
            gamma = sums[1] - facts[:, 2:3] * sums[2]
            beta = gamma / facts[:, 0:1]
            curvature = sums[0] + 2.0 * beta * sums[2] + beta * beta * facts[:, 1:2]
            alpha = gamma / curvature
            first, second = facts[:, 2:3] + alpha * beta, alpha
            step = got + beta * ins["step"][...]
            direction = grad + beta * ins["direction"][...]
            slip = ins["slip"][...] + alpha * direction
        fresh = grad - alpha * step
        out_bf[...] = fresh.astype(BF)
        for name, value in zip(NAMES, (fresh, step, direction, slip)):
            outs[name][...] = value
        lane = lax.broadcasted_iota(jnp.int32, (events, LANES), 1)
        out = jnp.zeros((events, LANES), F32)
        for n, value in enumerate((gamma, curvature, first, second, beta)):
            out = jnp.where(lane == n, value, out)
        outs["facts"][...] = out

    wide = jax.ShapeDtypeStruct((events, width), F32)
    shapes = [jax.ShapeDtypeStruct((events, width), BF), wide]
    if stage:
        shapes += [wide] * 3 + [jax.ShapeDtypeStruct((events, LANES), F32)]
    args = [summed, mask]
    if stage == 1:
        args.append(state["grad"])
    elif stage:
        args += [state[n] for n in NAMES]
    whole = lambda a: pl.BlockSpec(a.shape, lambda i: (0,) * len(a.shape))
    scratch = [pltpu.VMEM((events, total), F32)]
    outs = call(body, (1,), [whole(a) for a in args], [whole(s) for s in shapes], shapes, scratch=scratch)(*args)
    return outs[0], dict(zip(NAMES, outs[1:]))


def picked(place, waves, into):
    for at in range(BLOCKS):

        @pl.when(place == at)
        def _():
            for n, refs in enumerate(waves):
                into[n] = refs[at][...]


def whole_refs(flat):
    return [pl.BlockSpec(memory_space=pltpu.VMEM) for _ in flat]


def halfway(order, observed, mask, first, second, facts):
    events, gauges, times = observed.shape
    rows = events // BLOCKS
    halves = len(first)
    each = gauges // halves
    flat = [a for half in first + second for a in half]

    def body(order_ref, obs_ref, mask_ref, fact_ref, *refs):
        res_ref, wave_ref, block = refs[len(flat) :]
        groups = [refs[n * BLOCKS : (n + 1) * BLOCKS] for n in range(2 * halves)]
        picked(pl.program_id(0), groups, block)
        old = fact_ref[...]
        a, b, beta = old[:, 2:3], old[:, 3:4], old[:, 4:5]
        for h in range(halves):
            one, two = block[h].astype(F32), block[halves + h].astype(F32)
            cut = slice(h * each, (h + 1) * each)
            left = jnp.swapaxes(a[None] * one + b[None] * two, 0, 1)
            res_ref[:, cut] = obs_ref[:, cut] * mask_ref[cut][None, :, :1] - left
            wave_ref[:, cut] = jnp.swapaxes(two + beta[None] * one, 0, 1).astype(BF)

    natural = pl.BlockSpec((rows, gauges, times), lambda i, o: (o[i], 0, 0))
    shapes = [jax.ShapeDtypeStruct(observed.shape, kind) for kind in (F32, BF)]
    return call(
        body,
        (BLOCKS,),
        [
            natural,
            pl.BlockSpec((gauges, LANES), lambda i, o: (0, 0)),
            pl.BlockSpec((rows, LANES), lambda i, o: (i, 0)),
        ]
        + whole_refs(flat),
        [natural, natural],
        shapes,
        scratch=[pltpu.VMEM((2 * halves, each, rows, times), BF)],
        scalars=1,
    )(order, observed, mask, facts, *flat)


def turned(value):
    spare = LANES - value.shape[0]
    if spare:
        value = jnp.concatenate([value, jnp.zeros((spare, LANES), F32)], axis=0)
    return value.T


def last_sums(owns, others, facts):
    rows = owns[0].shape[1]
    groups = [owns] + others

    def body(*refs):
        out_ref, sum_ref = refs[-2:]
        halves = len(owns)
        sum_ref[...] = jnp.zeros_like(sum_ref)
        for h in range(halves):
            u = refs[h][...].astype(F32)
            for n in range(len(groups)):
                v = u * (u if n == 0 else refs[n * halves + h][...].astype(F32))
                v = folded(jnp.sum(v, axis=0))
                lane = lax.broadcasted_iota(jnp.int32, (rows, LANES), 1)
                sum_ref[...] += jnp.where(lane == n, jnp.sum(v, axis=1, keepdims=True), 0.0)
        out_ref[...] = turned(sum_ref[...])[:8]

    flat = [a for group in groups for a in group]
    return call(
        body,
        (1,),
        [pl.BlockSpec(a.shape, lambda i: (0, 0, 0)) for a in flat],
        pl.BlockSpec((8, LANES), lambda i: (0, 0)),
        jax.ShapeDtypeStruct((8, LANES), F32),
        scratch=[pltpu.VMEM((rows, LANES), F32)],
    )(*flat)


def last_factors(sums, facts):
    def body(sum_ref, fact_ref, out_ref):
        tot = jnp.sum(sum_ref[...], axis=0)
        old = turned(fact_ref[...])
        row = lambda a, n: a[n : n + 1]
        gamma = row(tot, 1) - row(old, 2) * row(tot, 2) - row(old, 3) * row(tot, 3)
        beta = gamma / row(old, 0)
        along = row(tot, 3) + row(old, 4) * row(tot, 2)
        alpha = gamma / (row(tot, 0) + 2.0 * beta * along + beta * beta * row(old, 1))
        out_ref[...] = jnp.zeros_like(out_ref)
        out_ref[0:1] = alpha
        out_ref[1:2] = beta

    return call(
        body,
        (1,),
        [pl.BlockSpec(sums.shape, lambda i: (0, 0, 0)), pl.BlockSpec((16, LANES), lambda i: (0, 0))],
        pl.BlockSpec((8, LANES), lambda i: (0, 0)),
        jax.ShapeDtypeStruct((8, LANES), F32),
    )(sums, facts)


def finished(order, news, res, prior, waves, state):
    events, gauges, times = res.shape
    rows = events // BLOCKS
    width = state["slip"].shape[1]
    halves = len(waves)
    each = gauges // halves
    flat = [a for half in waves for a in half]

    def body(order_ref, new_ref, res_ref, prior_ref, grad_ref, dir_ref, slip_ref, *refs):
        out_slip, out_res, block = refs[len(flat) :]
        groups = [refs[n * BLOCKS : (n + 1) * BLOCKS] for n in range(halves)]
        picked(pl.program_id(0), groups, block)
        new = turned(new_ref[0])[:rows]
        alpha, beta = new[:, 0:1], new[:, 1:2]
        out_slip[...] = slip_ref[...] + alpha * (grad_ref[...] + beta * dir_ref[...])
        alpha, both = alpha[:, :, None], (alpha * beta)[:, :, None]
        for h in range(halves):
            cut = slice(h * each, (h + 1) * each)
            wave = jnp.swapaxes(block[h].astype(F32) * new[:, 0:1][None], 0, 1)
            out_res[:, cut] = res_ref[:, cut] - wave - both * prior_ref[:, cut].astype(F32)

    natural = pl.BlockSpec((rows, gauges, times), lambda i, o: (o[i], 0, 0))
    small = pl.BlockSpec((rows, width), lambda i, o: (i, 0))
    return call(
        body,
        (BLOCKS,),
        [pl.BlockSpec((1, 8, LANES), lambda i, o: (o[i], 0, 0)), natural, natural, small, small, small]
        + whole_refs(flat),
        [pl.BlockSpec((rows, width), lambda i, o: (o[i], 0)), natural],
        [
            jax.ShapeDtypeStruct((events, width), F32),
            jax.ShapeDtypeStruct((events, gauges, times), F32),
        ],
        scratch=[pltpu.VMEM((halves, each, rows, times), BF)],
        scalars=1,
    )(order, news, res, prior, state["grad"], state["direction"], state["slip"], *flat)


HALVES = 1


def per_device(green, observed, gauge_mask, source_mask):
    x, core = lax.axis_index("x"), lax.axis_index("core")
    gauges, times, width = green.shape
    each = gauges // HALVES
    place = jnp.arange(BLOCKS, dtype=jnp.int32)
    order = (x - place % NX) % NX * NC + (core + place // NX) % NC

    wg = gauge_mask.astype(F32)
    wide_mask = jnp.broadcast_to(wg[:, None], (gauges, LANES))
    ps = source_mask.astype(F32)[None, :]
    wg, wide_mask, ps, order = lax.optimization_barrier((wg, wide_mask, ps, order))

    def predicted(vector):
        owns = []
        parts = [project(vector, green, h * each, each) for h in range(HALVES)]
        for h in range(HALVES):
            owns.append(source_sum(*parts[h], wg[h * each : (h + 1) * each, None, None]))
        return owns

    def shared(owns):
        return [with_core(along_x(own)) for own in owns]

    def gradient(waves, others):
        carry = None
        for h in range(HALVES):
            carry = gradient_parts(
                waves[h],
                green,
                h * each,
                each,
                [a if not isinstance(a, list) else a[h] for a in others],
                carry,
                h == HALVES - 1,
            )
        return gauge_sum(carry)

    start = reordered(observed, wide_mask, order)
    summed = gauge_sum(gradient_parts(start, green, 0, gauges))
    vector, state = renewed(0, summed, ps, None, width)

    first = shared(predicted(vector))
    vector, state = renewed(1, gradient(first, [start]), ps, state, width)
    second = shared(predicted(vector))
    vector, state = renewed(2, gradient(second, [start, first]), ps, state, width)
    owns = predicted(vector)

    res, prior = halfway(order, observed, wide_mask, first, second, state["facts"])
    others = [
        [start[0, h * each : (h + 1) * each] for h in range(HALVES)],
        [first[h][0] for h in range(HALVES)],
        [second[h][0] for h in range(HALVES)],
    ]
    near = [along_x(own) for own in owns]
    res, prior, others = lax.optimization_barrier((res, prior, others))
    sums = last_sums(owns, others, state["facts"])
    sums = sent_to_all(sums, GAUGE, PIECES)
    near, sums = lax.optimization_barrier((near, sums))
    third = [with_core(half) for half in near]
    factors = last_factors(sums, state["facts"])
    factors, third = lax.optimization_barrier((factors, third))
    news = sent_to_all(factors, ("x", "core"), BLOCKS)
    return tuple(finished(order, news, res, prior, third, state))


def solution(mesh):
    finer = Mesh(mesh.devices.reshape(NX, NC, NY, NZ), ("x", "core", "y", "z"))
    src = ("x", "core")
    in_specs = (P(GAUGE, None, src), P(None, GAUGE, None), P(GAUGE), P(src))
    out_specs = (P(None, src), P(None, GAUGE, None))
    return jax.shard_map(
        per_device, mesh=finer, in_specs=in_specs, out_specs=out_specs, check_vma=False
    )
```

```python
import jax
import jax.numpy as jnp
from jax import lax
from jax.experimental import pallas as pl
from jax.experimental.pallas import tpu as pltpu
from jax.sharding import Mesh
from jax.sharding import PartitionSpec as P


BF = jnp.bfloat16
F32 = jnp.float32
NX, NC, NY, NZ = 4, 2, 4, 8
BLOCKS = NX * NC
LANES = 128
GAUGE = ("y", "z")
PIECES = NY * NZ


def moved(value, axis, count, step):
    pairs = [(i, (i + step) % count) for i in range(count)]
    return lax.ppermute(value, axis, pairs)


def total_of(parts):
    total = parts[0].astype(F32)
    for part in parts[1:]:
        total = total + part.astype(F32)
    return total


def call(body, grid, in_specs, out_specs, out_shape, scratch=(), scalars=0, limit=20):
    return pl.pallas_call(
        body,
        grid_spec=pltpu.PrefetchScalarGridSpec(
            num_scalar_prefetch=scalars,
            grid=grid,
            in_specs=in_specs,
            out_specs=out_specs,
            scratch_shapes=list(scratch),
        ),
        out_shape=out_shape,
        compiler_params=pltpu.CompilerParams(vmem_limit_bytes=limit * 2**20),
    )


def reordered(observed, mask, order):
    rows, gauges, times = observed.shape[0] // BLOCKS, observed.shape[1], observed.shape[2]

    def body(order_ref, obs_ref, mask_ref, wave_ref):
        value = obs_ref[...] * mask_ref[...][None, :, :1]
        wave_ref[0] = jnp.swapaxes(value, 0, 1).astype(BF)

    return call(
        body,
        (BLOCKS,),
        [
            pl.BlockSpec((rows, gauges, times), lambda i, o: (o[i], 0, 0)),
            pl.BlockSpec((gauges, LANES), lambda i, o: (0, 0)),
        ],
        pl.BlockSpec((1, gauges, rows, times), lambda i, o: (i, 0, 0, 0)),
        jax.ShapeDtypeStruct((BLOCKS, gauges, rows, times), BF),
        scalars=1,
        limit=59,
    )(order, observed, mask)


def project(vector, green, start, gauges, step=4):
    _, times, width = green.shape
    rows = vector.shape[0] // BLOCKS
    first = start // step

    def body(vec_ref, green_ref, near_ref, far_ref):
        for g in range(step):
            part = lax.dot_general(
                vec_ref[...], green_ref[g], (((1,), (1,)), ((), ())), preferred_element_type=F32
            ).astype(BF)
            part = part.reshape(BLOCKS, rows, times)
            near_ref[:, g] = part[:NX]
            far_ref[:, g] = part[NX:]

    out = pl.BlockSpec((NX, step, rows, times), lambda i: (0, i, 0, 0))
    shape = jax.ShapeDtypeStruct((NX, gauges, rows, times), BF)
    return call(
        body,
        (gauges // step,),
        [
            pl.BlockSpec(vector.shape, lambda i: (0, 0)),
            pl.BlockSpec((step, times, width), lambda i: (first + i, 0, 0)),
        ],
        [out, out],
        [shape, shape],
    )(vector, green)


def split_two(value):
    high = value.astype(BF)
    return high, (value - high.astype(F32)).astype(BF)


def packed(sums):
    lane = lax.broadcasted_iota(jnp.int32, (sums[0].shape[0], LANES), 1)
    out = jnp.zeros(lane.shape, F32)
    for n, value in enumerate(sums):
        high, low = split_two(value)
        out = jnp.where(lane == 2 * n, high.astype(F32), out)
        out = jnp.where(lane == 2 * n + 1, low.astype(F32), out)
    return out


def folded(value):
    cuts = [value[..., t : t + LANES] for t in range(0, value.shape[-1], LANES)]
    return total_of(cuts)


def gradient_parts(waves, green, start, gauges, others=(), carry=None, last=True, step=4):
    _, times, width = green.shape
    first = start // step
    stacked = lambda a: not isinstance(a, list)
    rows = waves.shape[2] if stacked(waves) else waves[0].shape[1]
    events = BLOCKS * rows
    count = 1 + len(others) if others else 0
    args, specs = [], []

    def add(a):
        at = len(args)
        if stacked(a):
            args.append(a)
            specs.append(pl.BlockSpec((BLOCKS, step, rows, times), lambda i: (0, first + i, 0, 0)))
            return lambda refs, s, g: refs[at][s, g]
        args.extend(a)
        specs.extend([pl.BlockSpec((step, rows, times), lambda i: (i, 0, 0)) for _ in a])
        return lambda refs, s, g: refs[at + s][g]

    read = add(waves)
    reads = [add(a) for a in others]
    green_at = len(args)
    args.append(green)
    specs.append(pl.BlockSpec((step, times, width), lambda i: (first + i, 0, 0)))
    carry_at = len(args)
    acc_shape, sum_shape = (events, width), (max(count, 1), events, LANES)
    if carry is not None:
        args.extend(carry)
        specs.append(pl.BlockSpec(acc_shape, lambda i: (0, 0)))
        specs.append(pl.BlockSpec(sum_shape, lambda i: (0, 0, 0)))
    total = len(args)

    def body(*refs):
        if last:
            out_ref, acc_ref, sum_ref = refs[total:]
        else:
            acc_ref, sum_ref = refs[total:]

        @pl.when(pl.program_id(0) == 0)
        def _():
            if carry is not None:
                acc_ref[...] = refs[carry_at][...]
                sum_ref[...] = refs[carry_at + 1][...]
            else:
                acc_ref[...] = jnp.zeros_like(acc_ref)
                sum_ref[...] = jnp.zeros_like(sum_ref)

        acc = acc_ref[...]
        for g in range(step):
            wave = jnp.concatenate([read(refs, s, g) for s in range(BLOCKS)], axis=0)
            acc = acc + lax.dot_general(
                wave, refs[green_at][g], (((1,), (0,)), ((), ())), preferred_element_type=F32
            )
        acc_ref[...] = acc
        if count:

            @pl.loop(0, step)
            def _(g):
                for s in range(BLOCKS):
                    u = read(refs, s, g).astype(F32)
                    for n in range(count):
                        v = u * (u if n == 0 else reads[n - 1](refs, s, g).astype(F32))
                        sum_ref[n, s * rows : (s + 1) * rows, :] += folded(v)

        if last:

            @pl.when(pl.program_id(0) == gauges // step - 1)
            def _():
                if count:
                    sums = [jnp.sum(sum_ref[n], axis=1, keepdims=True) for n in range(count)]
                    sum_ref[0] = packed(sums)
                for q in range(PIECES):
                    at = slice(q * events // PIECES, (q + 1) * events // PIECES)
                    out_ref[q, :, :width] = acc_ref[at, :].astype(BF)
                    if count:
                        out_ref[q, :, width:] = sum_ref[0, at, :].astype(BF)

    acc_out = jax.ShapeDtypeStruct(acc_shape, F32)
    sum_out = jax.ShapeDtypeStruct(sum_shape, F32)
    wide = width + (LANES if count else 0)
    if last:
        out_specs = pl.BlockSpec((PIECES, events // PIECES, wide), lambda i: (0, 0, 0))
        out_shape = jax.ShapeDtypeStruct((PIECES, events // PIECES, wide), BF)
        scratch = [pltpu.VMEM(acc_shape, F32), pltpu.VMEM(sum_shape, F32)]
    else:
        out_specs = [
            pl.BlockSpec(acc_shape, lambda i: (0, 0)),
            pl.BlockSpec(sum_shape, lambda i: (0, 0, 0)),
        ]
        out_shape = [acc_out, sum_out]
        scratch = []
    return call(body, (gauges // step,), specs, out_specs, out_shape, scratch=scratch)(*args)


def sent_to_all(value, axes, count):
    wide = jnp.broadcast_to(value[None], (count, *value.shape))
    return lax.all_to_all(wide, axes, 0, 0, tiled=True)


def gauge_sum(pieces):
    got = lax.all_to_all(pieces, GAUGE, 0, 0, tiled=True)
    return sent_to_all(jnp.sum(got.astype(F32), axis=0), GAUGE, PIECES)


def source_sum(near, far, mask, beside):
    other = moved(far, "core", NC, 1)
    mine = [near[s].astype(F32) + other[s].astype(F32) for s in range(NX)]
    got = [mine[0]] + [moved(mine[s].astype(BF), "x", NX, -s) for s in range(1, NX)]
    if beside:
        got, beside = lax.optimization_barrier((got, beside))
    return (mask * total_of(got)).astype(BF), beside


def along_x(own):
    return [own] + [moved(own, "x", NX, s) for s in range(1, NX)]


def with_core(near):
    return near + [moved(value, "core", NC, 1) for value in near]


NAMES = ("grad", "step", "direction", "slip", "facts")


def renewed(stage, summed, mask, state, width):
    pieces, share, total = summed.shape
    events = pieces * share

    def body(*refs):
        refs = list(refs)
        sum_ref, mask_ref = refs.pop(0), refs.pop(0)
        ins = dict(zip(NAMES, [refs.pop(0) for _ in NAMES])) if stage > 1 else {}
        if stage == 1:
            ins = {"grad": refs.pop(0)}
        out_bf = refs.pop(0)
        joined = refs.pop()
        outs = dict(zip(NAMES, refs))
        for q in range(pieces):
            joined[q * share : (q + 1) * share, :] = sum_ref[q]
        got = joined[:, :width] * mask_ref[...].astype(F32)
        if stage == 0:
            out_bf[...] = got.astype(BF)
            outs["grad"][...] = got
            return
        tail = joined[:, width:]
        sums = [tail[:, 2 * n : 2 * n + 1] + tail[:, 2 * n + 1 : 2 * n + 2] for n in range(3)]
        grad = ins["grad"][...]
        if stage == 1:
            curvature, gamma = sums[0], sums[1]
            alpha = gamma / curvature
            beta = jnp.zeros_like(alpha)
            first, second = alpha, beta
            step, direction = got, grad
            slip = alpha * direction
        else:
            facts = ins["facts"][...]
            gamma = sums[1] - facts[:, 2:3] * sums[2]
            beta = gamma / facts[:, 0:1]
            curvature = sums[0] + 2.0 * beta * sums[2] + beta * beta * facts[:, 1:2]
            alpha = gamma / curvature
            first, second = facts[:, 2:3] + alpha * beta, alpha
            step = got + beta * ins["step"][...]
            direction = grad + beta * ins["direction"][...]
            slip = ins["slip"][...] + alpha * direction
        fresh = grad - alpha * step
        out_bf[...] = fresh.astype(BF)
        for name, value in zip(NAMES, (fresh, step, direction, slip)):
            outs[name][...] = value
        lane = lax.broadcasted_iota(jnp.int32, (events, LANES), 1)
        out = jnp.zeros((events, LANES), F32)
        for n, value in enumerate((gamma, curvature, first, second, beta)):
            out = jnp.where(lane == n, value, out)
        outs["facts"][...] = out

    wide = jax.ShapeDtypeStruct((events, width), F32)
    shapes = [jax.ShapeDtypeStruct((events, width), BF), wide]
    if stage:
        shapes += [wide] * 3 + [jax.ShapeDtypeStruct((events, LANES), F32)]
    args = [summed, mask]
    if stage == 1:
        args.append(state["grad"])
    elif stage:
        args += [state[n] for n in NAMES]
    whole = lambda a: pl.BlockSpec(a.shape, lambda i: (0,) * len(a.shape))
    scratch = [pltpu.VMEM((events, total), F32)]
    outs = call(body, (1,), [whole(a) for a in args], [whole(s) for s in shapes], shapes, scratch=scratch)(*args)
    return outs[0], dict(zip(NAMES, outs[1:]))


def picked(place, waves, into):
    for at in range(BLOCKS):

        @pl.when(place == at)
        def _():
            for n, refs in enumerate(waves):
                into[n] = refs[at][...]


def whole_refs(flat):
    return [pl.BlockSpec(memory_space=pltpu.VMEM) for _ in flat]


def halfway(order, observed, mask, first, second, facts):
    events, gauges, times = observed.shape
    rows = events // BLOCKS
    halves = len(first)
    each = gauges // halves
    flat = [a for half in first + second for a in half]

    def body(order_ref, obs_ref, mask_ref, fact_ref, *refs):
        res_ref, wave_ref, block = refs[len(flat) :]
        groups = [refs[n * BLOCKS : (n + 1) * BLOCKS] for n in range(2 * halves)]
        picked(pl.program_id(0), groups, block)
        old = fact_ref[...]
        a, b, beta = old[:, 2:3], old[:, 3:4], old[:, 4:5]
        for h in range(halves):
            one, two = block[h].astype(F32), block[halves + h].astype(F32)
            cut = slice(h * each, (h + 1) * each)
            left = jnp.swapaxes(a[None] * one + b[None] * two, 0, 1)
            res_ref[:, cut] = obs_ref[:, cut] * mask_ref[cut][None, :, :1] - left
            wave_ref[:, cut] = jnp.swapaxes(two + beta[None] * one, 0, 1).astype(BF)

    natural = pl.BlockSpec((rows, gauges, times), lambda i, o: (o[i], 0, 0))
    shapes = [jax.ShapeDtypeStruct(observed.shape, kind) for kind in (F32, BF)]
    return call(
        body,
        (BLOCKS,),
        [
            natural,
            pl.BlockSpec((gauges, LANES), lambda i, o: (0, 0)),
            pl.BlockSpec((rows, LANES), lambda i, o: (i, 0)),
        ]
        + whole_refs(flat),
        [natural, natural],
        shapes,
        scratch=[pltpu.VMEM((2 * halves, each, rows, times), BF)],
        scalars=1,
    )(order, observed, mask, facts, *flat)


def turned(value):
    spare = LANES - value.shape[0]
    if spare:
        value = jnp.concatenate([value, jnp.zeros((spare, LANES), F32)], axis=0)
    return value.T


def last_sums(owns, others, facts):
    rows = owns[0].shape[1]
    groups = [owns] + others

    def body(*refs):
        out_ref, sum_ref = refs[-2:]
        halves = len(owns)
        sum_ref[...] = jnp.zeros_like(sum_ref)
        for h in range(halves):
            u = refs[h][...].astype(F32)
            for n in range(len(groups)):
                v = u * (u if n == 0 else refs[n * halves + h][...].astype(F32))
                v = folded(jnp.sum(v, axis=0))
                lane = lax.broadcasted_iota(jnp.int32, (rows, LANES), 1)
                sum_ref[...] += jnp.where(lane == n, jnp.sum(v, axis=1, keepdims=True), 0.0)
        out_ref[...] = turned(sum_ref[...])[:8]

    flat = [a for group in groups for a in group]
    return call(
        body,
        (1,),
        [pl.BlockSpec(a.shape, lambda i: (0, 0, 0)) for a in flat],
        pl.BlockSpec((8, LANES), lambda i: (0, 0)),
        jax.ShapeDtypeStruct((8, LANES), F32),
        scratch=[pltpu.VMEM((rows, LANES), F32)],
    )(*flat)


def last_factors(sums, facts):
    def body(sum_ref, fact_ref, out_ref):
        tot = jnp.sum(sum_ref[...], axis=0)
        old = turned(fact_ref[...])
        row = lambda a, n: a[n : n + 1]
        gamma = row(tot, 1) - row(old, 2) * row(tot, 2) - row(old, 3) * row(tot, 3)
        beta = gamma / row(old, 0)
        along = row(tot, 3) + row(old, 4) * row(tot, 2)
        alpha = gamma / (row(tot, 0) + 2.0 * beta * along + beta * beta * row(old, 1))
        out_ref[...] = jnp.zeros_like(out_ref)
        out_ref[0:1] = alpha
        out_ref[1:2] = beta

    return call(
        body,
        (1,),
        [pl.BlockSpec(sums.shape, lambda i: (0, 0, 0)), pl.BlockSpec((16, LANES), lambda i: (0, 0))],
        pl.BlockSpec((8, LANES), lambda i: (0, 0)),
        jax.ShapeDtypeStruct((8, LANES), F32),
    )(sums, facts)


def finished(order, news, res, prior, waves, state):
    events, gauges, times = res.shape
    rows = events // BLOCKS
    width = state["slip"].shape[1]
    halves = len(waves)
    each = gauges // halves
    flat = [a for half in waves for a in half]

    def body(order_ref, new_ref, res_ref, prior_ref, grad_ref, dir_ref, slip_ref, *refs):
        out_slip, out_res, block = refs[len(flat) :]
        groups = [refs[n * BLOCKS : (n + 1) * BLOCKS] for n in range(halves)]
        picked(pl.program_id(0), groups, block)
        new = turned(new_ref[0])[:rows]
        alpha, beta = new[:, 0:1], new[:, 1:2]
        out_slip[...] = slip_ref[...] + alpha * (grad_ref[...] + beta * dir_ref[...])
        alpha, both = alpha[:, :, None], (alpha * beta)[:, :, None]
        for h in range(halves):
            cut = slice(h * each, (h + 1) * each)
            wave = jnp.swapaxes(block[h].astype(F32) * new[:, 0:1][None], 0, 1)
            out_res[:, cut] = res_ref[:, cut] - wave - both * prior_ref[:, cut].astype(F32)

    natural = pl.BlockSpec((rows, gauges, times), lambda i, o: (o[i], 0, 0))
    small = pl.BlockSpec((rows, width), lambda i, o: (i, 0))
    return call(
        body,
        (BLOCKS,),
        [pl.BlockSpec((1, 8, LANES), lambda i, o: (i, 0, 0)), natural, natural, small, small, small]
        + whole_refs(flat),
        [pl.BlockSpec((rows, width), lambda i, o: (o[i], 0)), natural],
        [
            jax.ShapeDtypeStruct((events, width), F32),
            jax.ShapeDtypeStruct((events, gauges, times), F32),
        ],
        scratch=[pltpu.VMEM((halves, each, rows, times), BF)],
        scalars=1,
    )(order, news, res, prior, state["grad"], state["direction"], state["slip"], *flat)


HALVES = 1


def per_device(green, observed, gauge_mask, source_mask):
    x, core = lax.axis_index("x"), lax.axis_index("core")
    gauges, times, width = green.shape
    each = gauges // HALVES
    place = jnp.arange(BLOCKS, dtype=jnp.int32)
    order = (x - place % NX) % NX * NC + (core + place // NX) % NC

    wg = gauge_mask.astype(F32)
    wide_mask = jnp.broadcast_to(wg[:, None], (gauges, LANES))
    ps = source_mask[None, :]
    wg, wide_mask, order = lax.optimization_barrier((wg, wide_mask, order))

    def predicted(vector, beside=()):
        owns = []
        parts = [project(vector, green, h * each, each) for h in range(HALVES)]
        for h in range(HALVES):
            own, beside = source_sum(*parts[h], wg[h * each : (h + 1) * each, None, None], beside)
            owns.append(own)
        return owns, beside

    def shared(owns):
        return [with_core(along_x(own)) for own in owns]

    def gradient(waves, others):
        carry = None
        for h in range(HALVES):
            carry = gradient_parts(
                waves[h],
                green,
                h * each,
                each,
                [a if not isinstance(a, list) else a[h] for a in others],
                carry,
                h == HALVES - 1,
            )
        return gauge_sum(carry)

    start = reordered(observed, wide_mask, order)
    summed = gauge_sum(gradient_parts(start, green, 0, gauges))
    vector, state = renewed(0, summed, ps, None, width)

    first = shared(predicted(vector)[0])
    vector, state = renewed(1, gradient(first, [start]), ps, state, width)
    second = shared(predicted(vector)[0])
    vector, state = renewed(2, gradient(second, [start, first]), ps, state, width)
    beside = halfway(order, observed, wide_mask, first, second, state["facts"])
    owns, (res, prior) = predicted(vector, tuple(beside))
    others = [
        [start[0, h * each : (h + 1) * each] for h in range(HALVES)],
        [first[h][0] for h in range(HALVES)],
        [second[h][0] for h in range(HALVES)],
    ]
    near = [along_x(own) for own in owns]
    sums = last_sums(owns, others, state["facts"])
    sums = sent_to_all(sums, GAUGE, PIECES)
    near, sums = lax.optimization_barrier((near, sums))
    third = [with_core(half) for half in near]
    factors = last_factors(sums, state["facts"])
    pair = jnp.stack([factors, moved(factors, "core", NC, 1)])
    pairs = jnp.stack(along_x(pair))
    news = jnp.swapaxes(pairs, 0, 1).reshape(BLOCKS, *factors.shape)
    return tuple(finished(order, news, res, prior, third, state))


def solution(mesh):
    finer = Mesh(mesh.devices.reshape(NX, NC, NY, NZ), ("x", "core", "y", "z"))
    src = ("x", "core")
    in_specs = (P(GAUGE, None, src), P(None, GAUGE, None), P(GAUGE), P(src))
    out_specs = (P(None, src), P(None, GAUGE, None))
    return jax.shard_map(
        per_device, mesh=finer, in_specs=in_specs, out_specs=out_specs, check_vma=False
    )
```

```python
import jax
import jax.numpy as jnp
from jax import lax
from jax.experimental import pallas as pl
from jax.experimental.pallas import tpu as pltpu
from jax.sharding import Mesh
from jax.sharding import PartitionSpec as P


BF = jnp.bfloat16
F32 = jnp.float32
NX, NC, NY, NZ = 4, 2, 4, 8
BLOCKS = NX * NC
LANES = 128
GAUGE = ("y", "z")
PIECES = NY * NZ


def moved(value, axis, count, step):
    pairs = [(i, (i + step) % count) for i in range(count)]
    return lax.ppermute(value, axis, pairs)


def total_of(parts):
    total = parts[0].astype(F32)
    for part in parts[1:]:
        total = total + part.astype(F32)
    return total


def call(body, grid, in_specs, out_specs, out_shape, scratch=(), scalars=0, limit=20):
    return pl.pallas_call(
        body,
        grid_spec=pltpu.PrefetchScalarGridSpec(
            num_scalar_prefetch=scalars,
            grid=grid,
            in_specs=in_specs,
            out_specs=out_specs,
            scratch_shapes=list(scratch),
        ),
        out_shape=out_shape,
        compiler_params=pltpu.CompilerParams(vmem_limit_bytes=limit * 2**20),
    )


def reordered(observed, mask, order):
    rows, gauges, times = observed.shape[0] // BLOCKS, observed.shape[1], observed.shape[2]

    def body(order_ref, obs_ref, mask_ref, wave_ref):
        value = obs_ref[...] * mask_ref[...][None, :, :1]
        wave_ref[0] = jnp.swapaxes(value, 0, 1).astype(BF)

    return call(
        body,
        (BLOCKS,),
        [
            pl.BlockSpec((rows, gauges, times), lambda i, o: (o[i], 0, 0)),
            pl.BlockSpec((gauges, LANES), lambda i, o: (0, 0)),
        ],
        pl.BlockSpec((1, gauges, rows, times), lambda i, o: (i, 0, 0, 0)),
        jax.ShapeDtypeStruct((BLOCKS, gauges, rows, times), BF),
        scalars=1,
    )(order, observed, mask)


def swapped(green):
    gauges, times, width = green.shape

    def body(green_ref, out_ref):
        out_ref[0] = green_ref[0].T

    return call(
        body,
        (gauges,),
        [pl.BlockSpec((1, times, width), lambda i: (i, 0, 0))],
        pl.BlockSpec((1, width, times), lambda i: (i, 0, 0)),
        jax.ShapeDtypeStruct((gauges, width, times), green.dtype),
    )(green)


def project(vector, green, start, gauges, along, step=4):
    times = green.shape[1 if along else 2]
    rows = vector.shape[0] // BLOCKS
    first = start // step

    def body(vec_ref, green_ref, near_ref, far_ref):
        for g in range(step):
            part = lax.dot_general(
                vec_ref[...], green_ref[g], (((1,), (along,)), ((), ())), preferred_element_type=F32
            ).astype(BF)
            part = part.reshape(BLOCKS, rows, times)
            near_ref[:, g] = part[:NX]
            far_ref[:, g] = part[NX:]

    out = pl.BlockSpec((NX, step, rows, times), lambda i: (0, i, 0, 0))
    shape = jax.ShapeDtypeStruct((NX, gauges, rows, times), BF)
    return call(
        body,
        (gauges // step,),
        [
            pl.BlockSpec(vector.shape, lambda i: (0, 0)),
            pl.BlockSpec((step, *green.shape[1:]), lambda i: (first + i, 0, 0)),
        ],
        [out, out],
        [shape, shape],
    )(vector, green)


def split_two(value):
    high = value.astype(BF)
    return high, (value - high.astype(F32)).astype(BF)


def packed(sums):
    lane = lax.broadcasted_iota(jnp.int32, (sums[0].shape[0], LANES), 1)
    out = jnp.zeros(lane.shape, F32)
    for n, value in enumerate(sums):
        high, low = split_two(value)
        out = jnp.where(lane == 2 * n, high.astype(F32), out)
        out = jnp.where(lane == 2 * n + 1, low.astype(F32), out)
    return out


def folded(value):
    cuts = [value[..., t : t + LANES] for t in range(0, value.shape[-1], LANES)]
    return total_of(cuts)


def gradient_parts(waves, green, start, gauges, others=(), carry=None, last=True, step=4):
    _, times, width = green.shape
    first = start // step
    stacked = lambda a: not isinstance(a, list)
    rows = waves.shape[2] if stacked(waves) else waves[0].shape[1]
    events = BLOCKS * rows
    count = 1 + len(others) if others else 0
    args, specs = [], []

    def add(a):
        at = len(args)
        if stacked(a):
            args.append(a)
            specs.append(pl.BlockSpec((BLOCKS, step, rows, times), lambda i: (0, first + i, 0, 0)))
            return lambda refs, s, g: refs[at][s, g]
        args.extend(a)
        specs.extend([pl.BlockSpec((step, rows, times), lambda i: (i, 0, 0)) for _ in a])
        return lambda refs, s, g: refs[at + s][g]

    read = add(waves)
    reads = [add(a) for a in others]
    green_at = len(args)
    args.append(green)
    specs.append(pl.BlockSpec((step, times, width), lambda i: (first + i, 0, 0)))
    carry_at = len(args)
    acc_shape, sum_shape = (events, width), (max(count, 1), events, LANES)
    if carry is not None:
        args.extend(carry)
        specs.append(pl.BlockSpec(acc_shape, lambda i: (0, 0)))
        specs.append(pl.BlockSpec(sum_shape, lambda i: (0, 0, 0)))
    total = len(args)

    def body(*refs):
        if last:
            out_ref, acc_ref, sum_ref = refs[total:]
        else:
            acc_ref, sum_ref = refs[total:]

        @pl.when(pl.program_id(0) == 0)
        def _():
            if carry is not None:
                acc_ref[...] = refs[carry_at][...]
                sum_ref[...] = refs[carry_at + 1][...]
            else:
                acc_ref[...] = jnp.zeros_like(acc_ref)
                sum_ref[...] = jnp.zeros_like(sum_ref)

        acc = acc_ref[...]
        for g in range(step):
            wave = jnp.concatenate([read(refs, s, g) for s in range(BLOCKS)], axis=0)
            acc = acc + lax.dot_general(
                wave, refs[green_at][g], (((1,), (0,)), ((), ())), preferred_element_type=F32
            )
        acc_ref[...] = acc
        if count:

            @pl.loop(0, step)
            def _(g):
                for s in range(BLOCKS):
                    u = read(refs, s, g).astype(F32)
                    for n in range(count):
                        v = u * (u if n == 0 else reads[n - 1](refs, s, g).astype(F32))
                        sum_ref[n, s * rows : (s + 1) * rows, :] += folded(v)

        if last:

            @pl.when(pl.program_id(0) == gauges // step - 1)
            def _():
                if count:
                    sums = [jnp.sum(sum_ref[n], axis=1, keepdims=True) for n in range(count)]
                    sum_ref[0] = packed(sums)
                for q in range(PIECES):
                    at = slice(q * events // PIECES, (q + 1) * events // PIECES)
                    out_ref[q, :, :width] = acc_ref[at, :].astype(BF)
                    if count:
                        out_ref[q, :, width:] = sum_ref[0, at, :].astype(BF)

    acc_out = jax.ShapeDtypeStruct(acc_shape, F32)
    sum_out = jax.ShapeDtypeStruct(sum_shape, F32)
    wide = width + (LANES if count else 0)
    if last:
        out_specs = pl.BlockSpec((PIECES, events // PIECES, wide), lambda i: (0, 0, 0))
        out_shape = jax.ShapeDtypeStruct((PIECES, events // PIECES, wide), BF)
        scratch = [pltpu.VMEM(acc_shape, F32), pltpu.VMEM(sum_shape, F32)]
    else:
        out_specs = [
            pl.BlockSpec(acc_shape, lambda i: (0, 0)),
            pl.BlockSpec(sum_shape, lambda i: (0, 0, 0)),
        ]
        out_shape = [acc_out, sum_out]
        scratch = []
    return call(body, (gauges // step,), specs, out_specs, out_shape, scratch=scratch)(*args)


def sent_to_all(value, axes, count):
    wide = jnp.broadcast_to(value[None], (count, *value.shape))
    return lax.all_to_all(wide, axes, 0, 0, tiled=True)


def gauge_sum(pieces):
    got = lax.all_to_all(pieces, GAUGE, 0, 0, tiled=True)
    return sent_to_all(jnp.sum(got.astype(F32), axis=0), GAUGE, PIECES)


def source_sum(near, far, mask, beside):
    other = moved(far, "core", NC, 1)
    mine = [near[s].astype(F32) + other[s].astype(F32) for s in range(NX)]
    got = [mine[0]] + [moved(mine[s].astype(BF), "x", NX, -s) for s in range(1, NX)]
    if beside:
        got, beside = lax.optimization_barrier((got, beside))
    return (mask * total_of(got)).astype(BF), beside


def along_x(own):
    return [own] + [moved(own, "x", NX, s) for s in range(1, NX)]


def with_core(near):
    return near + [moved(value, "core", NC, 1) for value in near]


NAMES = ("grad", "step", "direction", "slip", "facts")


def renewed(stage, summed, mask, state, width):
    pieces, share, total = summed.shape
    events = pieces * share

    def body(*refs):
        refs = list(refs)
        sum_ref, mask_ref = refs.pop(0), refs.pop(0)
        ins = dict(zip(NAMES, [refs.pop(0) for _ in NAMES])) if stage > 1 else {}
        if stage == 1:
            ins = {"grad": refs.pop(0)}
        out_bf = refs.pop(0)
        joined = refs.pop()
        outs = dict(zip(NAMES, refs))
        for q in range(pieces):
            joined[q * share : (q + 1) * share, :] = sum_ref[q]
        got = joined[:, :width] * mask_ref[...].astype(F32)
        if stage == 0:
            out_bf[...] = got.astype(BF)
            outs["grad"][...] = got
            return
        tail = joined[:, width:]
        sums = [tail[:, 2 * n : 2 * n + 1] + tail[:, 2 * n + 1 : 2 * n + 2] for n in range(3)]
        grad = ins["grad"][...]
        if stage == 1:
            curvature, gamma = sums[0], sums[1]
            alpha = gamma / curvature
            beta = jnp.zeros_like(alpha)
            first, second = alpha, beta
            step, direction = got, grad
            slip = alpha * direction
        else:
            facts = ins["facts"][...]
            gamma = sums[1] - facts[:, 2:3] * sums[2]
            beta = gamma / facts[:, 0:1]
            curvature = sums[0] + 2.0 * beta * sums[2] + beta * beta * facts[:, 1:2]
            alpha = gamma / curvature
            first, second = facts[:, 2:3] + alpha * beta, alpha
            step = got + beta * ins["step"][...]
            direction = grad + beta * ins["direction"][...]
            slip = ins["slip"][...] + alpha * direction
        fresh = grad - alpha * step
        out_bf[...] = fresh.astype(BF)
        for name, value in zip(NAMES, (fresh, step, direction, slip)):
            outs[name][...] = value
        lane = lax.broadcasted_iota(jnp.int32, (events, LANES), 1)
        out = jnp.zeros((events, LANES), F32)
        for n, value in enumerate((gamma, curvature, first, second, beta)):
            out = jnp.where(lane == n, value, out)
        outs["facts"][...] = out

    wide = jax.ShapeDtypeStruct((events, width), F32)
    shapes = [jax.ShapeDtypeStruct((events, width), BF), wide]
    if stage:
        shapes += [wide] * 3 + [jax.ShapeDtypeStruct((events, LANES), F32)]
    args = [summed, mask]
    if stage == 1:
        args.append(state["grad"])
    elif stage:
        args += [state[n] for n in NAMES]
    whole = lambda a: pl.BlockSpec(a.shape, lambda i: (0,) * len(a.shape))
    scratch = [pltpu.VMEM((events, total), F32)]
    outs = call(body, (1,), [whole(a) for a in args], [whole(s) for s in shapes], shapes, scratch=scratch)(*args)
    return outs[0], dict(zip(NAMES, outs[1:]))


def picked(place, waves, into):
    for at in range(BLOCKS):

        @pl.when(place == at)
        def _():
            for n, refs in enumerate(waves):
                into[n] = refs[at][...]


def whole_refs(flat):
    return [pl.BlockSpec(memory_space=pltpu.VMEM) for _ in flat]


def halfway(order, observed, mask, first, second, facts):
    events, gauges, times = observed.shape
    rows = events // BLOCKS
    halves = len(first)
    each = gauges // halves
    flat = [a for half in first + second for a in half]

    def body(order_ref, obs_ref, mask_ref, fact_ref, *refs):
        res_ref, wave_ref, block = refs[len(flat) :]
        groups = [refs[n * BLOCKS : (n + 1) * BLOCKS] for n in range(2 * halves)]
        picked(pl.program_id(0), groups, block)
        old = fact_ref[...]
        a, b, beta = old[:, 2:3], old[:, 3:4], old[:, 4:5]
        for h in range(halves):
            one, two = block[h].astype(F32), block[halves + h].astype(F32)
            cut = slice(h * each, (h + 1) * each)
            left = jnp.swapaxes(a[None] * one + b[None] * two, 0, 1)
            res_ref[:, cut] = obs_ref[:, cut] * mask_ref[cut][None, :, :1] - left
            wave_ref[:, cut] = jnp.swapaxes(two + beta[None] * one, 0, 1).astype(BF)

    natural = pl.BlockSpec((rows, gauges, times), lambda i, o: (o[i], 0, 0))
    shapes = [jax.ShapeDtypeStruct(observed.shape, kind) for kind in (F32, BF)]
    return call(
        body,
        (BLOCKS,),
        [
            natural,
            pl.BlockSpec((gauges, LANES), lambda i, o: (0, 0)),
            pl.BlockSpec((rows, LANES), lambda i, o: (i, 0)),
        ]
        + whole_refs(flat),
        [natural, natural],
        shapes,
        scratch=[pltpu.VMEM((2 * halves, each, rows, times), BF)],
        scalars=1,
    )(order, observed, mask, facts, *flat)


def turned(value):
    spare = LANES - value.shape[0]
    if spare:
        value = jnp.concatenate([value, jnp.zeros((spare, LANES), F32)], axis=0)
    return value.T


def last_sums(owns, others, facts):
    rows = owns[0].shape[1]
    groups = [owns] + others

    def body(*refs):
        out_ref, sum_ref = refs[-2:]
        halves = len(owns)
        sum_ref[...] = jnp.zeros_like(sum_ref)
        for h in range(halves):
            u = refs[h][...].astype(F32)
            for n in range(len(groups)):
                v = u * (u if n == 0 else refs[n * halves + h][...].astype(F32))
                v = folded(jnp.sum(v, axis=0))
                lane = lax.broadcasted_iota(jnp.int32, (rows, LANES), 1)
                sum_ref[...] += jnp.where(lane == n, jnp.sum(v, axis=1, keepdims=True), 0.0)
        out_ref[...] = turned(sum_ref[...])[:8]

    flat = [a for group in groups for a in group]
    return call(
        body,
        (1,),
        [pl.BlockSpec(a.shape, lambda i: (0, 0, 0)) for a in flat],
        pl.BlockSpec((8, LANES), lambda i: (0, 0)),
        jax.ShapeDtypeStruct((8, LANES), F32),
        scratch=[pltpu.VMEM((rows, LANES), F32)],
    )(*flat)


def last_factors(sums, facts):
    def body(sum_ref, fact_ref, out_ref):
        tot = jnp.sum(sum_ref[...], axis=0)
        old = turned(fact_ref[...])
        row = lambda a, n: a[n : n + 1]
        gamma = row(tot, 1) - row(old, 2) * row(tot, 2) - row(old, 3) * row(tot, 3)
        beta = gamma / row(old, 0)
        along = row(tot, 3) + row(old, 4) * row(tot, 2)
        alpha = gamma / (row(tot, 0) + 2.0 * beta * along + beta * beta * row(old, 1))
        out_ref[...] = jnp.zeros_like(out_ref)
        out_ref[0:1] = alpha
        out_ref[1:2] = beta

    return call(
        body,
        (1,),
        [pl.BlockSpec(sums.shape, lambda i: (0, 0, 0)), pl.BlockSpec((16, LANES), lambda i: (0, 0))],
        pl.BlockSpec((8, LANES), lambda i: (0, 0)),
        jax.ShapeDtypeStruct((8, LANES), F32),
    )(sums, facts)


def finished(order, news, res, prior, waves, state):
    events, gauges, times = res.shape
    rows = events // BLOCKS
    width = state["slip"].shape[1]
    halves = len(waves)
    each = gauges // halves
    flat = [a for half in waves for a in half]

    def body(order_ref, new_ref, res_ref, prior_ref, grad_ref, dir_ref, slip_ref, *refs):
        out_slip, out_res, block = refs[len(flat) :]
        groups = [refs[n * BLOCKS : (n + 1) * BLOCKS] for n in range(halves)]
        picked(pl.program_id(0), groups, block)
        new = turned(new_ref[0])[:rows]
        alpha, beta = new[:, 0:1], new[:, 1:2]
        out_slip[...] = slip_ref[...] + alpha * (grad_ref[...] + beta * dir_ref[...])
        alpha, both = alpha[:, :, None], (alpha * beta)[:, :, None]
        for h in range(halves):
            cut = slice(h * each, (h + 1) * each)
            wave = jnp.swapaxes(block[h].astype(F32) * new[:, 0:1][None], 0, 1)
            out_res[:, cut] = res_ref[:, cut] - wave - both * prior_ref[:, cut].astype(F32)

    natural = pl.BlockSpec((rows, gauges, times), lambda i, o: (o[i], 0, 0))
    small = pl.BlockSpec((rows, width), lambda i, o: (i, 0))
    return call(
        body,
        (BLOCKS,),
        [pl.BlockSpec((1, 8, LANES), lambda i, o: (i, 0, 0)), natural, natural, small, small, small]
        + whole_refs(flat),
        [pl.BlockSpec((rows, width), lambda i, o: (o[i], 0)), natural],
        [
            jax.ShapeDtypeStruct((events, width), F32),
            jax.ShapeDtypeStruct((events, gauges, times), F32),
        ],
        scratch=[pltpu.VMEM((halves, each, rows, times), BF)],
        scalars=1,
    )(order, news, res, prior, state["grad"], state["direction"], state["slip"], *flat)


HALVES = 1


def per_device(green, observed, gauge_mask, source_mask):
    x, core = lax.axis_index("x"), lax.axis_index("core")
    gauges, times, width = green.shape
    each = gauges // HALVES
    place = jnp.arange(BLOCKS, dtype=jnp.int32)
    order = (x - place % NX) % NX * NC + (core + place // NX) % NC

    wg = gauge_mask.astype(F32)
    wide_mask = jnp.broadcast_to(wg[:, None], (gauges, LANES))
    ps = source_mask[None, :]
    wg, wide_mask, order = lax.optimization_barrier((wg, wide_mask, order))

    def predicted(vector, table, along, beside):
        owns = []
        parts = [project(vector, table, h * each, each, along) for h in range(HALVES)]
        for h in range(HALVES):
            own, beside = source_sum(*parts[h], wg[h * each : (h + 1) * each, None, None], beside)
            owns.append(own)
        return owns, beside

    def shared(owns):
        return [with_core(along_x(own)) for own in owns]

    def gradient(waves, others):
        carry = None
        for h in range(HALVES):
            carry = gradient_parts(
                waves[h],
                green,
                h * each,
                each,
                [a if not isinstance(a, list) else a[h] for a in others],
                carry,
                h == HALVES - 1,
            )
        return gauge_sum(carry)

    start = reordered(observed, wide_mask, order)
    summed = gauge_sum(gradient_parts(start, green, 0, gauges))
    vector, state = renewed(0, summed, ps, None, width)

    owns, (table,) = predicted(vector, green, 1, (swapped(green),))
    first = shared(owns)
    vector, state = renewed(1, gradient(first, [start]), ps, state, width)
    second = shared(predicted(vector, table, 0, ())[0])
    vector, state = renewed(2, gradient(second, [start, first]), ps, state, width)
    beside = halfway(order, observed, wide_mask, first, second, state["facts"])
    owns, (res, prior) = predicted(vector, table, 0, tuple(beside))
    others = [
        [start[0, h * each : (h + 1) * each] for h in range(HALVES)],
        [first[h][0] for h in range(HALVES)],
        [second[h][0] for h in range(HALVES)],
    ]
    near = [along_x(own) for own in owns]
    sums = last_sums(owns, others, state["facts"])
    sums = sent_to_all(sums, GAUGE, PIECES)
    near, sums = lax.optimization_barrier((near, sums))
    third = [with_core(half) for half in near]
    factors = last_factors(sums, state["facts"])
    pair = jnp.stack([factors, moved(factors, "core", NC, 1)])
    pairs = jnp.stack(along_x(pair))
    news = jnp.swapaxes(pairs, 0, 1).reshape(BLOCKS, *factors.shape)
    return tuple(finished(order, news, res, prior, third, state))


def solution(mesh):
    finer = Mesh(mesh.devices.reshape(NX, NC, NY, NZ), ("x", "core", "y", "z"))
    src = ("x", "core")
    in_specs = (P(GAUGE, None, src), P(None, GAUGE, None), P(GAUGE), P(src))
    out_specs = (P(None, src), P(None, GAUGE, None))
    return jax.shard_map(
        per_device, mesh=finer, in_specs=in_specs, out_specs=out_specs, check_vma=False
    )
```
